32 devices in a mesh: region: 2 (over x), leaf: 16 (over z, y, core).
Axes of the slice: x: 2, y: 2, z: 4, core: 2. Of those that a mesh axis runs over, the one named last changes fastest.
Arguments:
- whiten: bfloat16 [32, 1024, 1024], P(('region', 'leaf')), as said below
- leaf_root: bfloat16 [32, 1024, 512], P(('region', 'leaf')), may hold values from -6 to 6
- leaf_region: bfloat16 [32, 1024, 512], P(('region', 'leaf')), may hold values from -6 to 6
- root_factor: bfloat16 [512, 512], P('region'), may hold values from -0.25 to 0.25
- root_adjoint: bfloat16 [512, 512], P('region'), may hold values from -0.25 to 0.25
- region_factor: bfloat16 [2, 512, 512], P('region', 'leaf'), may hold values from -0.25 to 0.25
- region_adjoint: bfloat16 [2, 512, 512], P('region', 'leaf'), may hold values from -0.25 to 0.25
Outputs:
- grad_root_basis: bfloat16 [32, 1024, 512], P(('region', 'leaf'))
- grad_region_basis: bfloat16 [32, 1024, 512], P(('region', 'leaf'))
- grad_root_factor: float32 [512, 512], P('leaf')
- grad_region_factor: float32 [2, 512, 512], P('region', 'leaf')
The draws below stay inside these ranges and needn't reach their ends.
Inputs may be any that keep to these rules, and one draw needn't show every extreme that they name: `whiten`: each whitening matrix is lower triangular with a positive diagonal.
All inputs are finite; a program needn't handle non-finite values.
Results may differ from the reference program's by a relative error of at most 0.018.
Values may be sent and summed in bfloat16 or wider, within the bound.
A program may use at most 64 MiB of HBM per device.

```python
import jax
import jax.numpy as jnp
from jax import lax

R = 512
M = 512
OBS = 1024
LEAVES = 32
REGIONS = 2


def draw_whiten(key, part):
    first, second = jax.random.split(jax.random.fold_in(key, 17))
    spread = 0.5 * jax.random.normal(first, (LEAVES, OBS, OBS), jnp.float32) / jnp.sqrt(OBS * 1.0)
    lower = jnp.tril(spread, -1)
    diag_vals = jnp.exp(jax.random.uniform(second, (LEAVES, OBS), jnp.float32, jnp.log(0.5), jnp.log(2.0)))
    eye_mat = jnp.eye(OBS, dtype=jnp.float32)
    return (lower + diag_vals[:, :, None] * eye_mat[None]).astype(jnp.bfloat16)


def block_levels(key, extent, shards, least, high):
    level, own = 1.0, jax.random.fold_in(key, 6)
    for position, blocks in shards:
        heights = jnp.exp(jax.random.uniform(jax.random.fold_in(own, position), (blocks,), jnp.float32, least / len(shards), high / len(shards)))
        level = level * jnp.repeat(heights, extent[position] // blocks).reshape([-1 if axis == position else 1 for axis in range(len(extent))])
    return level


def centred(own_key, extent, deviation, bound, cuts=(), held_as=jnp.bfloat16):
    array = deviation * jax.random.normal(own_key, extent, jnp.float32)
    if cuts:
        array = array * block_levels(own_key, extent, cuts, -0.22, 0.18)
    return jnp.clip(array, -bound, bound).astype(held_as)


def setup_inputs(seed: int = 0) -> dict:
    keys = jax.random.split(jax.random.key(seed), 8)
    return {
        "whiten": draw_whiten(jax.random.fold_in(keys[7], 71), 0),
        "leaf_root": centred(keys[1], (LEAVES, OBS, R), 1.0, 6.0, ((0, 32),)),
        "leaf_region": centred(keys[2], (LEAVES, OBS, M), 1.0, 6.0, ((0, 32),)),
        "root_factor": centred(keys[3], (R, R), R ** -0.5, 0.25, ((0, 2),)),
        "root_adjoint": centred(keys[4], (R, R), R ** -0.5, 0.25, ((0, 2),)),
        "region_factor": centred(keys[5], (REGIONS, M, M), M ** -0.5, 0.25, ((0, 2), (1, 16))),
        "region_adjoint": centred(keys[6], (REGIONS, M, M), M ** -0.5, 0.25, ((0, 2), (1, 16))),
    }


def matmul(left, right):
    return jnp.dot(left.astype(jnp.float32), right.astype(jnp.float32), preferred_element_type=jnp.float32)


def reference(whiten, leaf_root, leaf_region, root_factor, root_adjoint, region_factor, region_adjoint):
    root_wide = root_adjoint.astype(jnp.float32)
    region_wide = region_adjoint.astype(jnp.float32)
    root_sym = (root_wide + root_wide.T).astype(jnp.bfloat16)
    region_sym = (region_wide + jnp.swapaxes(region_wide, 1, 2)).astype(jnp.bfloat16)
    per_region = LEAVES // REGIONS

    def visit(carry, inputs):
        root_total, region_total = carry
        factor_inv, base_root, base_region, number = inputs
        owner = (number // per_region).astype(jnp.int32)
        own_factor = lax.dynamic_index_in_dim(region_factor, owner, 0, keepdims=False)
        own_sym = lax.dynamic_index_in_dim(region_sym, owner, 0, keepdims=False)
        root_basis = matmul(base_root, root_factor).astype(jnp.bfloat16)
        region_basis = matmul(base_region, own_factor).astype(jnp.bfloat16)
        root_white = matmul(factor_inv, root_basis).astype(jnp.bfloat16)
        region_white = matmul(factor_inv, region_basis).astype(jnp.bfloat16)
        root_dwhite = matmul(root_white, root_sym).astype(jnp.bfloat16)
        region_dwhite = matmul(region_white, own_sym).astype(jnp.bfloat16)
        grad_root = matmul(factor_inv.T, root_dwhite).astype(jnp.bfloat16)
        grad_region = matmul(factor_inv.T, region_dwhite).astype(jnp.bfloat16)
        root_total = root_total + matmul(base_root.T, grad_root) / OBS
        region_term = matmul(base_region.T, grad_region) / OBS
        old = lax.dynamic_index_in_dim(region_total, owner, 0, keepdims=True)
        region_total = lax.dynamic_update_index_in_dim(region_total, old + region_term[None], owner, 0)
        return (root_total, region_total), (grad_root, grad_region)

    start = (jnp.zeros((R, R), jnp.float32), jnp.zeros((REGIONS, M, M), jnp.float32))
    numbers = jnp.arange(LEAVES, dtype=jnp.int32)
    (root_total, region_total), (grad_root_basis, grad_region_basis) = lax.scan(
        visit, start, (whiten, leaf_root, leaf_region, numbers))
    return grad_root_basis, grad_region_basis, root_total, region_total
```

```python
import functools
import math

import jax
import jax.numpy as jnp
from jax import lax
from jax.experimental import pallas as pl
from jax.experimental.pallas import tpu as pltpu
from jax.sharding import PartitionSpec as P

MESH = pl.DeviceIdType.MESH
F32, BF16 = jnp.float32, jnp.bfloat16


def split_leaf(leaves):
    chips = leaves // 2
    fast = max(d for d in range(1, math.isqrt(chips) + 1) if chips % d == 0)
    return chips // fast, fast


def offset(value, step, count):
    if count & (count - 1):
        return lax.rem(value + step, count), lax.rem(value + count - step, count)
    bit = 1
    pair = value
    while bit < count:
        if step & bit:
            pair = pair + bit - 2 * bit * lax.rem(value // bit, 2)
        bit *= 2
    return pair, pair


def dot(left, right):
    return jnp.dot(left, right, preferred_element_type=F32)


def kernel(
    nr, nl,
    w_in, lr_in, lg_in, rf_in, ra_in, gf_in, ga_in,
    gr_out, gg_out, fr_out, fg_out,
    w, l, a, b, rt, rg, g, cb, rc, ys, ry, zs, rz, rx,
    ld, gz_s, gz_r, gy_s, gy_r, gc_s, gc_r, gx_s, gx_r, gp_s, gp_r,
    cs_s, cs_r, ys_s, ys_r, zs_s, zs_r, xs_s, xs_r,
):
    Z, Y = split_leaf(nl)
    obs, K = l.shape[1], l.shape[2]
    rows, half = K // nl, K // nr
    T = min(256, K)
    nb = obs // T
    r, leaf = lax.axis_index("region"), lax.axis_index("leaf")
    c, y, z = lax.rem(leaf, 2), lax.rem(leaf // 2, Y), leaf // (2 * Y)
    oc = 1 - c

    def at(zz, yy, cc):
        return (zz * Y + yy) * 2 + cc

    def zp(k):
        return offset(z, k, Z)[0]

    def zm(k):
        return offset(z, k, Z)[1]

    def yp(k):
        return offset(y, k, Y)[0]

    def ym(k):
        return offset(y, k, Y)[1]

    def rp(k):
        return lax.rem(r + k, nr)

    def rm(k):
        return lax.rem(r + nr - k, nr)

    def span(index, size):
        return pl.ds(pl.multiple_of(index * size, size), size)

    mine = span(leaf, rows)
    own = span(r, half)
    loads = [
        pltpu.make_async_copy(gf_in.at[0], rg.at[0, mine], ld.at[0]),
        pltpu.make_async_copy(ga_in.at[0], rg.at[1, mine], ld.at[1]),
        pltpu.make_async_copy(rf_in, rt.at[0, own], ld.at[2]),
        pltpu.make_async_copy(ra_in, rt.at[1, own], ld.at[3]),
        pltpu.make_async_copy(lr_in.at[0], l.at[0], ld.at[4]),
        pltpu.make_async_copy(w_in.at[0], w, ld.at[5]),
        pltpu.make_async_copy(lg_in.at[0], l.at[1], ld.at[6]),
    ]
    for load in loads:
        load.start()

    barrier = pltpu.get_barrier_semaphore()
    peers = [{"leaf": at(zp(k), y, c)} for k in range(1, Z)]
    peers += [{"leaf": at(z, yp(k), c)} for k in range(1, Y)]
    peers += [{"leaf": at(z, y, oc)}]
    peers += [{"region": rp(k)} for k in range(1, nr)]
    for peer in peers:
        pl.semaphore_signal(barrier, inc=1, device_id=peer, device_id_type=MESH)
    for load in loads[:4]:
        load.wait()
    pl.semaphore_wait(barrier, len(peers))

    sends = []

    def remote(src, dst, ssem, rsem, peer):
        return pltpu.make_async_remote_copy(
            src_ref=src, dst_ref=dst, send_sem=ssem, recv_sem=rsem,
            device_id=peer, device_id_type=MESH,
        )

    def send(src, dst, ssem, rsem, peer):
        copy = remote(src, dst, ssem, rsem, peer)
        copy.start()
        sends.append(copy)

    def arrive(ref, ssem, rsem, peer):
        remote(ref, ref, ssem, rsem, peer).wait_recv()

    other = {"leaf": at(z, y, oc)}

    def block(kz, ky, cc):
        return rg.at[:, span(at(zm(kz), ym(ky), cc), rows)]

    def gather_y(kz):
        for ky in range(1, Y):
            i = (ky - 1) * Z + kz
            send(block(kz, 0, c), block(kz, 0, c), gy_s.at[i], gy_r.at[i], {"leaf": at(z, yp(ky), c)})

    def gather_core(kz, ky):
        i = ky * Z + kz
        send(block(kz, ky, c), block(kz, ky, c), gc_s.at[i], gc_r.at[i], other)

    def z_forward(kz):
        arrive(block(kz, 0, c), gz_s.at[kz - 1], gz_r.at[kz - 1], other)
        gather_y(kz)
        gather_core(kz, 0)

    def y_forward(kz, ky):
        i = (ky - 1) * Z + kz
        arrive(block(kz, ky, c), gy_s.at[i], gy_r.at[i], other)
        gather_core(kz, ky)

    for k in range(1, Z):
        send(block(0, 0, c), block(0, 0, c), gz_s.at[k - 1], gz_r.at[k - 1], {"leaf": at(zp(k), y, c)})
    gather_y(0)
    for k in range(1, nr):
        send(rt.at[c, own], rt.at[c, own], gx_s.at[k - 1], gx_r.at[k - 1], {"region": rp(k)})
    gather_core(0, 0)

    scale = 1.0 / obs

    def local_a(p):
        for n in range(K // T):
            cols = pl.ds(n * T, T)
            for i in range(nb):
                a[p, pl.ds(i * T, T), cols] = dot(
                    w[pl.ds(i * T, T), pl.ds(0, (i + 1) * T)], l[p, pl.ds(0, (i + 1) * T), cols]
                ).astype(BF16)

    def local_c(p):
        per = T // (2 * Y * rows) if T >= 2 * Y * rows else 0
        step = T if per else 2 * Y * rows
        per = step // (2 * Y * rows)
        for i in range(K // step):
            left = a[p, :, pl.ds(i * step, step)].T
            part = (dot(left, a[p]) * scale).astype(BF16)
            cb[p, pl.ds(i * per, per)] = part.reshape(per, Y, 2, rows, K)
        send(cb.at[p, :, :, oc], rc.at[p], cs_s.at[p], cs_r.at[p], other)

    def local_b(i):
        left = w[pl.ds(i * T, obs - i * T), pl.ds(i * T, T)].T
        for p in range(2):
            b[p, pl.ds(i * T, T), :] = dot(left, a[p, pl.ds(i * T, obs - i * T), :]).astype(BF16)

    far = range(Z - 1, -1, -1)

    def reduce_y(p):
        arrive(rc.at[p], cs_s.at[p], cs_r.at[p], other)
        for kz in far:
            zz = zp(kz)
            for k in range(1, Y):
                yy = yp(k)
                ys[p, k - 1, kz] = (cb[p, zz, yy, c].astype(F32) + rc[p, zz, yy].astype(F32)).astype(BF16)
                i = (p * Y + k) * Z + kz
                send(ys.at[p, k - 1, kz], ry.at[p, k - 1, kz], ys_s.at[i], ys_r.at[i], {"leaf": at(z, yy, c)})

    def chip_sum(p, kz):
        zz = zp(kz)
        total = cb[p, zz, y, c].astype(F32) + rc[p, zz, y].astype(F32)
        for k in range(1, Y):
            i = (p * Y + k) * Z + kz
            arrive(ry.at[p, k - 1, kz], ys_s.at[i], ys_r.at[i], other)
            total += ry[p, k - 1, kz].astype(F32)
        return total

    def reduce_z(p):
        for k in far[:-1]:
            zs[p, k - 1] = chip_sum(p, k).astype(BF16)
            i = p * Z + k
            send(zs.at[p, k - 1], rz.at[p, k - 1], zs_s.at[i], zs_r.at[i], {"leaf": at(zp(k), y, c)})

    def finish_z(p):
        total = chip_sum(p, 0)
        for k in range(1, Z):
            i = p * Z + k
            arrive(rz.at[p, k - 1], zs_s.at[i], zs_r.at[i], other)
            total += rz[p, k - 1].astype(F32)
        return total

    def make_g(p, held):
        factor, adjoint = held[0], held[1]
        both = dot(factor, adjoint) + lax.dot_general(
            factor, adjoint, (((1,), (1,)), ((), ())), preferred_element_type=F32
        )
        g[p] = both.astype(BF16)

    def make_grad(p, out):
        for i in range(nb):
            part = pl.ds(i * T, T)
            out[0, part, :] = dot(b[p, part, :], g[p]).astype(BF16)

    loads[4].wait()
    loads[5].wait()
    local_a(0)
    local_c(0)
    if Z > 1:
        z_forward(1)
    loads[6].wait()
    local_a(1)
    local_c(1)
    if Z > 2:
        z_forward(2)
    local_b(0)
    reduce_y(0)
    for k in range(3, Z):
        z_forward(k)
    reduce_y(1)
    for i in range(1, nb):
        local_b(i)
    for ky in range(1, Y):
        y_forward(0, ky)
    reduce_z(0)
    for k in range(1, nr):
        theirs = rt.at[c, span(rm(k), half)]
        arrive(theirs, gx_s.at[k - 1], gx_r.at[k - 1], other)
        send(theirs, theirs, gp_s.at[k - 1], gp_r.at[k - 1], other)
    for ky in range(1, Y):
        for k in range(1, Z):
            y_forward(k, ky)
    reduce_z(1)
    for k in range(1, nr):
        arrive(rt.at[oc, span(rm(k), half)], gp_s.at[k - 1], gp_r.at[k - 1], other)
    make_g(0, rt)
    rx[r] = finish_z(0).astype(BF16)
    for k in range(1, nr):
        send(rx.at[r], rx.at[r], xs_s.at[k - 1], xs_r.at[k - 1], {"region": rp(k)})
    make_grad(0, gr_out)
    for ky in range(Y):
        for kz in range(Z):
            i = ky * Z + kz
            arrive(block(kz, ky, oc), gc_s.at[i], gc_r.at[i], other)
    make_g(1, rg)
    make_grad(1, gg_out)
    fg_out[0] = dot(finish_z(1).astype(BF16), g[1])
    for k in range(1, nr):
        arrive(rx.at[rm(k)], xs_s.at[k - 1], xs_r.at[k - 1], other)
    total = rx[0].astype(F32)
    for k in range(1, nr):
        total += rx[k].astype(F32)
    fr_out[...] = dot(total.astype(BF16), g[0])
    for copy in sends:
        copy.wait_send()


def store(*refs):
    held, target, store_sem = refs[:4], refs[4:8], refs[8]
    stores = [pltpu.make_async_copy(held[n], target[n], store_sem.at[n]) for n in range(4)]
    for save in stores:
        save.start()
    for save in stores:
        save.wait()


def solution(mesh):
    nr, nl = mesh.shape["region"], mesh.shape["leaf"]
    Z, Y = split_leaf(nl)

    def on_device(whiten, leaf_root, leaf_region, root_factor, root_adjoint, region_factor, region_adjoint):
        obs, K = leaf_root.shape[1], leaf_root.shape[2]
        rows = K // nl
        dma = lambda n: pltpu.SemaphoreType.DMA((max(n, 1),))
        args = [pltpu.with_memory_space_constraint(x, pltpu.HBM) for x in (
            whiten, leaf_root, leaf_region, root_factor, root_adjoint, region_factor, region_adjoint)]
        held = pl.pallas_call(
            functools.partial(kernel, nr, nl),
            out_shape=(
                jax.ShapeDtypeStruct(leaf_root.shape, BF16),
                jax.ShapeDtypeStruct(leaf_region.shape, BF16),
                jax.ShapeDtypeStruct((rows, K), F32),
                jax.ShapeDtypeStruct((1, rows, K), F32),
            ),
            in_specs=[pl.BlockSpec(memory_space=pltpu.HBM)] * 7,
            out_specs=(pl.BlockSpec(memory_space=pltpu.VMEM),) * 4,
            scratch_shapes=[
                pltpu.VMEM((obs, obs), BF16),
                pltpu.VMEM((2, obs, K), BF16),
                pltpu.VMEM((2, obs, K), BF16),
                pltpu.VMEM((2, obs, K), BF16),
                pltpu.VMEM((2, K, K), BF16),
                pltpu.VMEM((2, K, K), BF16),
                pltpu.VMEM((2, K, K), BF16),
                pltpu.VMEM((2, Z, Y, 2, rows, K), BF16),
                pltpu.VMEM((2, Z, Y, rows, K), BF16),
                pltpu.VMEM((2, max(Y - 1, 1), Z, rows, K), BF16),
                pltpu.VMEM((2, max(Y - 1, 1), Z, rows, K), BF16),
                pltpu.VMEM((2, max(Z - 1, 1), rows, K), BF16),
                pltpu.VMEM((2, max(Z - 1, 1), rows, K), BF16),
                pltpu.VMEM((nr, rows, K), BF16),
                dma(7),
                dma(Z - 1), dma(Z - 1),
                dma((Y - 1) * Z), dma((Y - 1) * Z),
                dma(Y * Z), dma(Y * Z),
                dma(nr - 1), dma(nr - 1),
                dma(nr - 1), dma(nr - 1),
                dma(2), dma(2),
                dma(2 * Y * Z), dma(2 * Y * Z),
                dma(2 * Z), dma(2 * Z),
                dma(nr - 1), dma(nr - 1),
            ],
            compiler_params=pltpu.CompilerParams(
                collective_id=0, has_side_effects=True, vmem_limit_bytes=40 << 20
            ),
            name="likelihood_backward",
        )(*args)
        return pl.pallas_call(
            store,
            out_shape=tuple(jax.ShapeDtypeStruct(x.shape, x.dtype) for x in held),
            in_specs=[pl.BlockSpec(memory_space=pltpu.VMEM)] * 4,
            out_specs=(pl.BlockSpec(memory_space=pltpu.HBM),) * 4,
            scratch_shapes=[dma(4)],
            compiler_params=pltpu.CompilerParams(vmem_limit_bytes=1 << 20),
            name="store_outputs",
        )(*held)

    return jax.shard_map(
        on_device,
        mesh=mesh,
        in_specs=(
            P(("region", "leaf"), None, None),
            P(("region", "leaf"), None, None),
            P(("region", "leaf"), None, None),
            P("region", None),
            P("region", None),
            P("region", "leaf", None),
            P("region", "leaf", None),
        ),
        out_specs=(
            P(("region", "leaf"), None, None),
            P(("region", "leaf"), None, None),
            P("leaf", None),
            P("region", "leaf", None),
        ),
        check_vma=False,
    )
```

```python
import functools
import math

import jax
import jax.numpy as jnp
from jax import lax
from jax.experimental import pallas as pl
from jax.experimental.pallas import tpu as pltpu
from jax.sharding import PartitionSpec as P

MESH = pl.DeviceIdType.MESH
F32, BF16 = jnp.float32, jnp.bfloat16


def split_leaf(leaves):
    chips = leaves // 2
    fast = max(d for d in range(1, math.isqrt(chips) + 1) if chips % d == 0)
    return chips // fast, fast


def offset(value, step, count):
    if count & (count - 1):
        return lax.rem(value + step, count), lax.rem(value + count - step, count)
    bit = 1
    pair = value
    while bit < count:
        if step & bit:
            pair = pair + bit - 2 * bit * lax.rem(value // bit, 2)
        bit *= 2
    return pair, pair


def dot(left, right):
    return jnp.dot(left, right, preferred_element_type=F32)


def kernel(
    nr, nl,
    w_in, lr_in, lg_in, rf_in, ra_in, gf_in, ga_in,
    gr_out, gg_out, fr_out, fg_out,
    w, l, a, b, rt, rg, g, cb, rc, ys, ry, zs, rz, rx,
    ld, lb, gz_s, gz_r, gy_s, gy_r, gc_s, gc_r, gx_s, gx_r, gp_s, gp_r,
    cs_s, cs_r, ys_s, ys_r, zs_s, zs_r, xs_s, xs_r, zn, yn, cn, xn,
):
    Z, Y = split_leaf(nl)
    obs, K = l.shape[1], l.shape[2]
    rows, half = K // nl, K // nr
    T = min(256, K)
    nb = obs // T
    r, leaf = lax.axis_index("region"), lax.axis_index("leaf")
    c, y, z = lax.rem(leaf, 2), lax.rem(leaf // 2, Y), leaf // (2 * Y)
    oc = 1 - c

    def at(zz, yy, cc):
        return (zz * Y + yy) * 2 + cc

    def zp(k):
        return offset(z, k, Z)[0]

    def zm(k):
        return offset(z, k, Z)[1]

    def yp(k):
        return offset(y, k, Y)[0]

    def ym(k):
        return offset(y, k, Y)[1]

    def rp(k):
        return lax.rem(r + k, nr)

    def rm(k):
        return lax.rem(r + nr - k, nr)

    def back(k, count):
        return count - k if count & (count - 1) else k

    def span(index, size):
        return pl.ds(pl.multiple_of(index * size, size), size)

    mine = span(leaf, rows)
    own = span(r, half)
    first = [
        pltpu.make_async_copy(gf_in.at[0], rg.at[0, mine], ld.at[0]),
        pltpu.make_async_copy(ga_in.at[0], rg.at[1, mine], ld.at[1]),
    ]
    halves = [
        pltpu.make_async_copy(rf_in, rt.at[0, own], ld.at[2]),
        pltpu.make_async_copy(ra_in, rt.at[1, own], ld.at[3]),
    ]
    bands = []
    for i in range(nb):
        band, left = pl.ds(i * T, T), pl.ds(0, (i + 1) * T)
        bands.append([
            pltpu.make_async_copy(w_in.at[0, band, left], w.at[band, left], lb.at[0, i]),
            pltpu.make_async_copy(lr_in.at[0, band], l.at[0, band], lb.at[1, i]),
        ])
    second = pltpu.make_async_copy(lg_in.at[0], l.at[1], ld.at[4])
    for load in first + sum(bands, []) + halves + [second]:
        load.start()

    other = {"leaf": at(z, y, oc)}
    z_peers = [({"leaf": at(zp(k), y, c)}, zp(k) > z, zn.at[k - 1], zn.at[back(k, Z) - 1]) for k in range(1, Z)]
    y_peers = [({"leaf": at(z, yp(k), c)}, yp(k) > y, yn.at[k - 1], yn.at[back(k, Y) - 1]) for k in range(1, Y)]
    x_peers = [({"region": rp(k)}, rp(k) > r, xn.at[k - 1], xn.at[nr - k - 1]) for k in range(1, nr)]
    c_peers = [(other, oc > c, cn.at[0], cn.at[0])]
    peers = z_peers + y_peers + x_peers + c_peers

    barrier = pltpu.get_barrier_semaphore()
    for peer, later, _, _ in peers:
        @pl.when(later)
        def _():
            pl.semaphore_signal(barrier, inc=1, device_id=peer, device_id_type=MESH)
    pl.when(leaf + r > 0)(lambda: pl.semaphore_wait(barrier, z + y + r + c))
    for peer, later, _, theirs in peers:
        @pl.when(jnp.logical_not(later))
        def _():
            pl.semaphore_signal(theirs, inc=1, device_id=peer, device_id_type=MESH)

    sends = []

    def remote(src, dst, ssem, rsem, peer):
        return pltpu.make_async_remote_copy(
            src_ref=src, dst_ref=dst, send_sem=ssem, recv_sem=rsem,
            device_id=peer, device_id_type=MESH,
        )

    def plan(src, dst, ssem, rsem, peer):
        copy = remote(src, dst, ssem, rsem, peer)
        sends.append(copy)
        return copy

    def send(*args):
        plan(*args).start()

    def arrive(ref, ssem, rsem):
        remote(ref, ref, ssem, rsem, other).wait_recv()

    def block(kz, ky, cc):
        return rg.at[:, span(at(zm(kz), ym(ky), cc), rows)]

    def gather_y(kz):
        return [
            (plan(block(kz, 0, c), block(kz, 0, c), gy_s.at[(ky - 1) * Z + kz], gy_r.at[(ky - 1) * Z + kz],
                  {"leaf": at(z, yp(ky), c)}))
            for ky in range(1, Y)
        ]

    def gather_core(kz, ky):
        i = ky * Z + kz
        return plan(block(kz, ky, c), block(kz, ky, c), gc_s.at[i], gc_r.at[i], other)

    def z_forward(kz):
        arrive(block(kz, 0, c), gz_s.at[kz - 1], gz_r.at[kz - 1])
        for copy in gather_y(kz):
            copy.start()
        gather_core(kz, 0).start()

    def y_forward(kz, ky):
        i = (ky - 1) * Z + kz
        arrive(block(kz, ky, c), gy_s.at[i], gy_r.at[i])
        gather_core(kz, ky).start()

    to_z = [plan(block(0, 0, c), block(0, 0, c), gz_s.at[k - 1], gz_r.at[k - 1], z_peers[k - 1][0]) for k in range(1, Z)]
    to_y = gather_y(0)
    to_c = [gather_core(0, 0)]
    to_x = [plan(rt.at[c, own], rt.at[c, own], gx_s.at[k - 1], gx_r.at[k - 1], x_peers[k - 1][0]) for k in range(1, nr)]

    def open_early(group, copies):
        for (_, later, _, _), copy in zip(group, copies):
            pl.when(jnp.logical_not(later))(copy.start)

    def open_late(group, copies):
        for (_, later, sem, _), copy in zip(group, copies):
            @pl.when(later)
            def _():
                pl.semaphore_wait(sem, 1)
                copy.start()

    scale = 1.0 / obs

    def a_band(p, i):
        a[p, pl.ds(i * T, T), :] = dot(
            w[pl.ds(i * T, T), pl.ds(0, (i + 1) * T)], l[p, pl.ds(0, (i + 1) * T), :]
        ).astype(BF16)

    step = max(T, 2 * Y * rows)
    per = step // (2 * Y * rows)
    parts = K // step

    def local_c(p):
        for i in range(parts):
            left = a[p, :, pl.ds(i * step, step)].T
            part = (dot(left, a[p]) * scale).astype(BF16)
            here = pl.ds(i * per, per)
            cb[p, here] = part.reshape(per, Y, 2, rows, K)
            send(cb.at[p, here, :, oc], rc.at[p, here], cs_s.at[p * parts + i], cs_r.at[p * parts + i], other)

    def local_b(i):
        left = w[pl.ds(i * T, obs - i * T), pl.ds(i * T, T)].T
        for p in range(2):
            b[p, pl.ds(i * T, T), :] = dot(left, a[p, pl.ds(i * T, obs - i * T), :]).astype(BF16)

    far = range(Z - 1, -1, -1)
    y_sends = {}
    for p in range(2):
        for kz in far:
            for k in range(1, Y):
                i = (p * Y + k) * Z + kz
                y_sends[p, kz, k] = plan(
                    ys.at[p, k - 1, kz], ry.at[p, k - 1, kz], ys_s.at[i], ys_r.at[i], {"leaf": at(z, yp(k), c)}
                )

    def reduce_y(p):
        for i in range(parts):
            arrive(rc.at[p, pl.ds(i * per, per)], cs_s.at[p * parts + i], cs_r.at[p * parts + i])
        for kz in far:
            zz = zp(kz)
            for k in range(1, Y):
                yy = yp(k)
                ys[p, k - 1, kz] = (cb[p, zz, yy, c].astype(F32) + rc[p, zz, yy].astype(F32)).astype(BF16)
                y_sends[p, kz, k].start()

    def chip_sum(p, kz):
        zz = zp(kz)
        total = cb[p, zz, y, c].astype(F32) + rc[p, zz, y].astype(F32)
        for k in range(1, Y):
            i = (p * Y + k) * Z + kz
            arrive(ry.at[p, k - 1, kz], ys_s.at[i], ys_r.at[i])
            total += ry[p, k - 1, kz].astype(F32)
        return total

    def reduce_z(p):
        for k in far[:-1]:
            zs[p, k - 1] = chip_sum(p, k).astype(BF16)
            i = p * Z + k
            send(zs.at[p, k - 1], rz.at[p, k - 1], zs_s.at[i], zs_r.at[i], {"leaf": at(zp(k), y, c)})

    def finish_z(p):
        total = chip_sum(p, 0)
        for k in range(1, Z):
            i = p * Z + k
            arrive(rz.at[p, k - 1], zs_s.at[i], zs_r.at[i])
            total += rz[p, k - 1].astype(F32)
        return total

    def make_g(p, held):
        factor, adjoint = held[0], held[1]
        both = dot(factor, adjoint) + lax.dot_general(
            factor, adjoint, (((1,), (1,)), ((), ())), preferred_element_type=F32
        )
        g[p] = both.astype(BF16)

    def make_grad(p, out):
        for i in range(nb):
            part = pl.ds(i * T, T)
            out[0, part, :] = dot(b[p, part, :], g[p]).astype(BF16)

    for load in first:
        load.wait()
    open_early(z_peers, to_z)
    open_early(y_peers, to_y)
    open_early(c_peers, to_c)
    for i in range(nb):
        for load in bands[i]:
            load.wait()
        a_band(0, i)
    open_late(c_peers, to_c)
    local_c(0)
    for load in halves:
        load.wait()
    open_early(x_peers, to_x)
    open_late(y_peers, to_y)
    open_late(z_peers, to_z)
    open_late(x_peers, to_x)
    pl.when(c == 1)(lambda: reduce_y(0))
    second.wait()
    for i in range(nb):
        a_band(1, i)
    local_c(1)
    pl.when(c == 1)(lambda: reduce_y(1))
    if Z > 1:
        z_forward(1)
    pl.when(c == 0)(lambda: reduce_y(0))
    if Z > 2:
        z_forward(2)
    local_b(0)
    for k in range(3, Z):
        z_forward(k)
    pl.when(c == 0)(lambda: reduce_y(1))
    for i in range(1, nb):
        local_b(i)
    for ky in range(1, Y):
        y_forward(0, ky)
    reduce_z(0)
    for k in range(1, nr):
        theirs = rt.at[c, span(rm(k), half)]
        arrive(theirs, gx_s.at[k - 1], gx_r.at[k - 1])
        send(theirs, theirs, gp_s.at[k - 1], gp_r.at[k - 1], other)
    for ky in range(1, Y):
        for k in range(1, Z):
            y_forward(k, ky)
    reduce_z(1)
    for k in range(1, nr):
        arrive(rt.at[oc, span(rm(k), half)], gp_s.at[k - 1], gp_r.at[k - 1])
    make_g(0, rt)
    rx[r] = finish_z(0).astype(BF16)
    for k in range(1, nr):
        send(rx.at[r], rx.at[r], xs_s.at[k - 1], xs_r.at[k - 1], {"region": rp(k)})
    make_grad(0, gr_out)
    for ky in range(Y):
        for kz in range(Z):
            i = ky * Z + kz
            arrive(block(kz, ky, oc), gc_s.at[i], gc_r.at[i])
    make_g(1, rg)
    make_grad(1, gg_out)
    fg_out[0] = dot(finish_z(1).astype(BF16), g[1])
    for k in range(1, nr):
        arrive(rx.at[rm(k)], xs_s.at[k - 1], xs_r.at[k - 1])
    total = rx[0].astype(F32)
    for k in range(1, nr):
        total += rx[k].astype(F32)
    fr_out[...] = dot(total.astype(BF16), g[0])
    for copy in sends:
        copy.wait_send()


def store(*refs):
    held, target, store_sem = refs[:4], refs[4:8], refs[8]
    stores = [pltpu.make_async_copy(held[n], target[n], store_sem.at[n]) for n in range(4)]
    for save in stores:
        save.start()
    for save in stores:
        save.wait()


def solution(mesh):
    nr, nl = mesh.shape["region"], mesh.shape["leaf"]
    Z, Y = split_leaf(nl)

    def on_device(whiten, leaf_root, leaf_region, root_factor, root_adjoint, region_factor, region_adjoint):
        obs, K = leaf_root.shape[1], leaf_root.shape[2]
        rows = K // nl
        parts = K // max(min(256, K), 2 * Y * rows)
        dma = lambda n: pltpu.SemaphoreType.DMA((max(n, 1),))
        flag = lambda n: pltpu.SemaphoreType.REGULAR((max(n, 1),))
        args = [pltpu.with_memory_space_constraint(x, pltpu.HBM) for x in (
            whiten, leaf_root, leaf_region, root_factor, root_adjoint, region_factor, region_adjoint)]
        held = pl.pallas_call(
            functools.partial(kernel, nr, nl),
            out_shape=(
                jax.ShapeDtypeStruct(leaf_root.shape, BF16),
                jax.ShapeDtypeStruct(leaf_region.shape, BF16),
                jax.ShapeDtypeStruct((rows, K), F32),
                jax.ShapeDtypeStruct((1, rows, K), F32),
            ),
            in_specs=[pl.BlockSpec(memory_space=pltpu.HBM)] * 7,
            out_specs=(pl.BlockSpec(memory_space=pltpu.VMEM),) * 4,
            scratch_shapes=[
                pltpu.VMEM((obs, obs), BF16),
                pltpu.VMEM((2, obs, K), BF16),
                pltpu.VMEM((2, obs, K), BF16),
                pltpu.VMEM((2, obs, K), BF16),
                pltpu.VMEM((2, K, K), BF16),
                pltpu.VMEM((2, K, K), BF16),
                pltpu.VMEM((2, K, K), BF16),
                pltpu.VMEM((2, Z, Y, 2, rows, K), BF16),
                pltpu.VMEM((2, Z, Y, rows, K), BF16),
                pltpu.VMEM((2, max(Y - 1, 1), Z, rows, K), BF16),
                pltpu.VMEM((2, max(Y - 1, 1), Z, rows, K), BF16),
                pltpu.VMEM((2, max(Z - 1, 1), rows, K), BF16),
                pltpu.VMEM((2, max(Z - 1, 1), rows, K), BF16),
                pltpu.VMEM((nr, rows, K), BF16),
                dma(5), pltpu.SemaphoreType.DMA((2, obs // min(256, K))),
                dma(Z - 1), dma(Z - 1),
                dma((Y - 1) * Z), dma((Y - 1) * Z),
                dma(Y * Z), dma(Y * Z),
                dma(nr - 1), dma(nr - 1),
                dma(nr - 1), dma(nr - 1),
                dma(2 * parts), dma(2 * parts),
                dma(2 * Y * Z), dma(2 * Y * Z),
                dma(2 * Z), dma(2 * Z),
                dma(nr - 1), dma(nr - 1),
                flag(Z - 1), flag(Y - 1), flag(1), flag(nr - 1),
            ],
            compiler_params=pltpu.CompilerParams(
                collective_id=0, has_side_effects=True, vmem_limit_bytes=40 << 20
            ),
            name="likelihood_backward",
        )(*args)
        return pl.pallas_call(
            store,
            out_shape=tuple(jax.ShapeDtypeStruct(x.shape, x.dtype) for x in held),
            in_specs=[pl.BlockSpec(memory_space=pltpu.VMEM)] * 4,
            out_specs=(pl.BlockSpec(memory_space=pltpu.HBM),) * 4,
            scratch_shapes=[dma(4)],
            compiler_params=pltpu.CompilerParams(vmem_limit_bytes=1 << 20),
            name="store_outputs",
        )(*held)

    return jax.shard_map(
        on_device,
        mesh=mesh,
        in_specs=(
            P(("region", "leaf"), None, None),
            P(("region", "leaf"), None, None),
            P(("region", "leaf"), None, None),
            P("region", None),
            P("region", None),
            P("region", "leaf", None),
            P("region", "leaf", None),
        ),
        out_specs=(
            P(("region", "leaf"), None, None),
            P(("region", "leaf"), None, None),
            P("leaf", None),
            P("region", "leaf", None),
        ),
        check_vma=False,
    )
```

```python
import functools
import math

import jax
import jax.numpy as jnp
from jax import lax
from jax.experimental import pallas as pl
from jax.experimental.pallas import tpu as pltpu
from jax.sharding import PartitionSpec as P

MESH = pl.DeviceIdType.MESH
F32, BF16 = jnp.float32, jnp.bfloat16


def split_leaf(leaves):
    chips = leaves // 2
    fast = max(d for d in range(1, math.isqrt(chips) + 1) if chips % d == 0)
    return chips // fast, fast


def offset(value, step, count):
    if count & (count - 1):
        return lax.rem(value + step, count), lax.rem(value + count - step, count)
    bit = 1
    pair = value
    while bit < count:
        if step & bit:
            pair = pair + bit - 2 * bit * lax.rem(value // bit, 2)
        bit *= 2
    return pair, pair


def dot(left, right):
    return jnp.dot(left, right, preferred_element_type=F32)


def kernel(
    nr, nl,
    w_in, lr_in, lg_in, rf_in, ra_in, gf_in, ga_in,
    gr_out, gg_out, fr_out, fg_out,
    w, l, a, b, rt, rg, g, cb, rc, ys, ry, zs, rz, rx,
    ld, lb, out_sem, gz, gy, gc, gx, gp, cs, yr, zr, xr, zn, yn, cn, xn,
):
    Z, Y = split_leaf(nl)
    obs, K = l.shape[1], l.shape[2]
    rows, half = K // nl, K // nr
    T = min(256, K)
    nb = obs // T
    r, leaf = lax.axis_index("region"), lax.axis_index("leaf")
    c, y, z = lax.rem(leaf, 2), lax.rem(leaf // 2, Y), leaf // (2 * Y)
    oc = 1 - c

    def at(zz, yy, cc):
        return (zz * Y + yy) * 2 + cc

    def zp(k):
        return offset(z, k, Z)[0]

    def zm(k):
        return offset(z, k, Z)[1]

    def yp(k):
        return offset(y, k, Y)[0]

    def ym(k):
        return offset(y, k, Y)[1]

    def rp(k):
        return lax.rem(r + k, nr)

    def rm(k):
        return lax.rem(r + nr - k, nr)

    def back(k, count):
        return count - k if count & (count - 1) else k

    def span(index, size):
        return pl.ds(pl.multiple_of(index * size, size), size)

    mine = span(leaf, rows)
    own = span(r, half)
    def copies(sem, *pairs):
        return [pltpu.make_async_copy(src, dst, sem) for src, dst in pairs]

    first = copies(ld.at[0], (gf_in.at[0], rg.at[0, mine]), (ga_in.at[0], rg.at[1, mine]))
    halves = copies(ld.at[1], (rf_in, rt.at[0, own]), (ra_in, rt.at[1, own]))
    bands = []
    for i in range(nb):
        band, left = pl.ds(i * T, T), pl.ds(0, (i + 1) * T)
        bands.append(copies(lb.at[i], (w_in.at[0, band, left], w.at[band, left]), (lr_in.at[0, band], l.at[0, band])))
    second = copies(ld.at[2], (lg_in.at[0], l.at[1]))
    for load in first + sum(bands, []) + halves + second:
        load.start()

    def taken(sem, count):
        whole = l.at[0, pl.ds(0, count)] if count <= obs else l.at[:, pl.ds(0, count // 2)]
        pltpu.make_async_copy(whole, whole, sem).wait()

    other = {"leaf": at(z, y, oc)}
    z_peers = [({"leaf": at(zp(k), y, c)}, zp(k) > z, zn.at[k - 1], zn.at[back(k, Z) - 1]) for k in range(1, Z)]
    y_peers = [({"leaf": at(z, yp(k), c)}, yp(k) > y, yn.at[k - 1], yn.at[back(k, Y) - 1]) for k in range(1, Y)]
    x_peers = [({"region": rp(k)}, rp(k) > r, xn.at[k - 1], xn.at[nr - k - 1]) for k in range(1, nr)]
    c_peers = [(other, oc > c, cn.at[0], cn.at[0])]
    peers = z_peers + y_peers + x_peers + c_peers

    barrier = pltpu.get_barrier_semaphore()
    for peer, later, _, _ in peers:
        @pl.when(later)
        def _():
            pl.semaphore_signal(barrier, inc=1, device_id=peer, device_id_type=MESH)
    pl.when(leaf + r > 0)(lambda: pl.semaphore_wait(barrier, z + y + r + c))
    for peer, later, _, theirs in peers:
        @pl.when(jnp.logical_not(later))
        def _():
            pl.semaphore_signal(theirs, inc=1, device_id=peer, device_id_type=MESH)

    sent = [0, 0]

    def plan(kind, src, dst, rsem, peer):
        sent[kind] += math.prod(src.shape) // K
        return pltpu.make_async_remote_copy(
            src_ref=src, dst_ref=dst, send_sem=out_sem.at[kind], recv_sem=rsem,
            device_id=peer, device_id_type=MESH,
        )

    def send(*args):
        plan(*args).start()

    def block(kz, ky, cc):
        return rg.at[:, span(at(zm(kz), ym(ky), cc), rows)]

    def to_ys(kz):
        return [
            plan(0, block(kz, 0, c), block(kz, 0, c), gy.at[(k - 1) * Z + kz], {"leaf": at(z, yp(k), c)})
            for k in range(1, Y)
        ]

    def to_core(kz, ky):
        return plan(0, block(kz, ky, c), block(kz, ky, c), gc.at[0], other)

    def from_z(kz):
        taken(gz.at[kz - 1], 2 * rows)
        for copy in to_ys(kz) + [to_core(kz, 0)]:
            copy.start()

    def from_y(kz, ky):
        taken(gy.at[(ky - 1) * Z + kz], 2 * rows)
        to_core(kz, ky).start()

    to_z = [plan(0, block(0, 0, c), block(0, 0, c), gz.at[k - 1], z_peers[k - 1][0]) for k in range(1, Z)]
    to_y = to_ys(0)
    to_c = [to_core(0, 0)]
    to_x = [plan(0, rt.at[c, own], rt.at[c, own], gx.at[k - 1], x_peers[k - 1][0]) for k in range(1, nr)]

    def open_early(group, copies):
        for (_, later, _, _), copy in zip(group, copies):
            pl.when(jnp.logical_not(later))(copy.start)

    def open_late(group, copies):
        for (_, later, sem, _), copy in zip(group, copies):
            @pl.when(later)
            def _():
                pl.semaphore_wait(sem, 1)
                copy.start()

    scale = 1.0 / obs

    def a_band(p, i):
        a[p, pl.ds(i * T, T), :] = dot(
            w[pl.ds(i * T, T), pl.ds(0, (i + 1) * T)], l[p, pl.ds(0, (i + 1) * T), :]
        ).astype(BF16)

    step = max(T, 2 * Y * rows)
    per = step // (2 * Y * rows)
    parts = K // step

    def local_c(p):
        for i in range(parts):
            left = a[p, :, pl.ds(i * step, step)].T
            part = (dot(left, a[p]) * scale).astype(BF16)
            here = pl.ds(i * per, per)
            cb[p, here] = part.reshape(per, Y, 2, rows, K)
            send(1, cb.at[p, here, :, oc], rc.at[p, here], cs.at[p], other)

    def local_b(i):
        left = w[pl.ds(i * T, obs - i * T), pl.ds(i * T, T)].T
        for p in range(2):
            b[p, pl.ds(i * T, T), :] = dot(left, a[p, pl.ds(i * T, obs - i * T), :]).astype(BF16)

    far = range(Z - 1, -1, -1)

    def reduce_y(p):
        taken(cs.at[p], K // 2)
        for kz in far:
            zz = zp(kz)
            for k in range(1, Y):
                yy = yp(k)
                ys[p, k - 1, kz] = (cb[p, zz, yy, c].astype(F32) + rc[p, zz, yy].astype(F32)).astype(BF16)
                send(1, ys.at[p, k - 1, kz], ry.at[p, k - 1, kz], yr.at[p * Z + kz], {"leaf": at(z, yy, c)})

    def chip_sum(p, kz):
        zz = zp(kz)
        total = cb[p, zz, y, c].astype(F32) + rc[p, zz, y].astype(F32)
        if Y > 1:
            taken(yr.at[p * Z + kz], (Y - 1) * rows)
        for k in range(1, Y):
            total += ry[p, k - 1, kz].astype(F32)
        return total

    def reduce_z(p):
        for k in far[:-1]:
            zs[p, k - 1] = chip_sum(p, k).astype(BF16)
            send(1, zs.at[p, k - 1], rz.at[p, k - 1], zr.at[p], {"leaf": at(zp(k), y, c)})

    def finish_z(p):
        total = chip_sum(p, 0)
        if Z > 1:
            taken(zr.at[p], (Z - 1) * rows)
        for k in range(1, Z):
            total += rz[p, k - 1].astype(F32)
        return total

    def make_g(p, held):
        adjoint = held[1].astype(F32)
        g[p] = dot(held[0], (adjoint + adjoint.T).astype(BF16)).astype(BF16)

    def make_grad(p, out):
        for i in range(nb):
            part = pl.ds(i * T, T)
            out[0, part, :] = dot(b[p, part, :], g[p]).astype(BF16)

    taken(ld.at[0], 2 * rows)
    open_early(y_peers, to_y)
    open_early(z_peers, to_z)
    open_early(c_peers, to_c)
    for i in range(nb):
        taken(lb.at[i], (i + 1) * T * T // K + T)
        a_band(0, i)
    open_late(c_peers, to_c)
    open_late(y_peers, to_y)
    open_late(z_peers, to_z)
    local_c(0)
    taken(ld.at[1], 2 * half)
    open_early(x_peers, to_x)
    open_late(x_peers, to_x)
    taken(ld.at[2], obs)
    for i in range(nb):
        a_band(1, i)
    reduce_y(0)
    local_c(1)
    local_b(0)
    reduce_y(1)
    for k in range(1, max(Z, nb)):
        if k < Z:
            from_z(k)
        if k < nb:
            local_b(k)
    reduce_z(0)
    for ky in range(1, Y):
        from_y(0, ky)
    for k in range(1, nr):
        theirs = rt.at[c, span(rm(k), half)]
        taken(gx.at[k - 1], half)
        send(0, theirs, theirs, gp.at[0], other)
    if nr > 1:
        taken(gp.at[0], (nr - 1) * half)
    make_g(0, rt)
    reduce_z(1)
    make_grad(0, gr_out)
    rx[r] = finish_z(0).astype(BF16)
    for k in range(1, nr):
        send(1, rx.at[r], rx.at[r], xr.at[0], {"region": rp(k)})
    for ky in range(1, Y):
        for k in range(1, Z):
            from_y(k, ky)
    taken(gc.at[0], K)
    make_g(1, rg)
    make_grad(1, gg_out)
    fg_out[0] = dot(finish_z(1).astype(BF16), g[1])
    if nr > 1:
        taken(xr.at[0], (nr - 1) * rows)
    total = rx[0].astype(F32)
    for k in range(1, nr):
        total += rx[k].astype(F32)
    fr_out[...] = dot(total.astype(BF16), g[0])
    for kind in range(2):
        taken(out_sem.at[kind], sent[kind])


def store(*refs):
    held, target, store_sem = refs[:4], refs[4:8], refs[8]
    stores = [pltpu.make_async_copy(held[n], target[n], store_sem.at[n]) for n in range(4)]
    for save in stores:
        save.start()
    for save in stores:
        save.wait()


def solution(mesh):
    nr, nl = mesh.shape["region"], mesh.shape["leaf"]
    Z, Y = split_leaf(nl)

    def on_device(whiten, leaf_root, leaf_region, root_factor, root_adjoint, region_factor, region_adjoint):
        obs, K = leaf_root.shape[1], leaf_root.shape[2]
        rows = K // nl
        dma = lambda n: pltpu.SemaphoreType.DMA((max(n, 1),))
        flag = lambda n: pltpu.SemaphoreType.REGULAR((max(n, 1),))
        args = [pltpu.with_memory_space_constraint(x, pltpu.HBM) for x in (
            whiten, leaf_root, leaf_region, root_factor, root_adjoint, region_factor, region_adjoint)]
        held = pl.pallas_call(
            functools.partial(kernel, nr, nl),
            out_shape=(
                jax.ShapeDtypeStruct(leaf_root.shape, BF16),
                jax.ShapeDtypeStruct(leaf_region.shape, BF16),
                jax.ShapeDtypeStruct((rows, K), F32),
                jax.ShapeDtypeStruct((1, rows, K), F32),
            ),
            in_specs=[pl.BlockSpec(memory_space=pltpu.HBM)] * 7,
            out_specs=(pl.BlockSpec(memory_space=pltpu.VMEM),) * 4,
            scratch_shapes=[
                pltpu.VMEM((obs, obs), BF16),
                pltpu.VMEM((2, obs, K), BF16),
                pltpu.VMEM((2, obs, K), BF16),
                pltpu.VMEM((2, obs, K), BF16),
                pltpu.VMEM((2, K, K), BF16),
                pltpu.VMEM((2, K, K), BF16),
                pltpu.VMEM((2, K, K), BF16),
                pltpu.VMEM((2, Z, Y, 2, rows, K), BF16),
                pltpu.VMEM((2, Z, Y, rows, K), BF16),
                pltpu.VMEM((2, max(Y - 1, 1), Z, rows, K), BF16),
                pltpu.VMEM((2, max(Y - 1, 1), Z, rows, K), BF16),
                pltpu.VMEM((2, max(Z - 1, 1), rows, K), BF16),
                pltpu.VMEM((2, max(Z - 1, 1), rows, K), BF16),
                pltpu.VMEM((nr, rows, K), BF16),
                dma(3), dma(obs // min(256, K)), dma(2),
                dma(Z - 1), dma((Y - 1) * Z), dma(1), dma(nr - 1), dma(1), dma(2), dma(2 * Z), dma(2), dma(1),
                flag(Z - 1), flag(Y - 1), flag(1), flag(nr - 1),
            ],
            compiler_params=pltpu.CompilerParams(
                collective_id=0, has_side_effects=True, vmem_limit_bytes=40 << 20
            ),
            name="likelihood_backward",
        )(*args)
        return pl.pallas_call(
            store,
            out_shape=tuple(jax.ShapeDtypeStruct(x.shape, x.dtype) for x in held),
            in_specs=[pl.BlockSpec(memory_space=pltpu.VMEM)] * 4,
            out_specs=(pl.BlockSpec(memory_space=pltpu.HBM),) * 4,
            scratch_shapes=[dma(4)],
            compiler_params=pltpu.CompilerParams(vmem_limit_bytes=1 << 20),
            name="store_outputs",
        )(*held)

    return jax.shard_map(
        on_device,
        mesh=mesh,
        in_specs=(
            P(("region", "leaf"), None, None),
            P(("region", "leaf"), None, None),
            P(("region", "leaf"), None, None),
            P("region", None),
            P("region", None),
            P("region", "leaf", None),
            P("region", "leaf", None),
        ),
        out_specs=(
            P(("region", "leaf"), None, None),
            P(("region", "leaf"), None, None),
            P("leaf", None),
            P("region", "leaf", None),
        ),
        check_vma=False,
    )
```

```python
import functools
import math

import jax
import jax.numpy as jnp
from jax import lax
from jax.experimental import pallas as pl
from jax.experimental.pallas import tpu as pltpu
from jax.sharding import PartitionSpec as P

MESH = pl.DeviceIdType.MESH
F32, BF16 = jnp.float32, jnp.bfloat16


def split_leaf(leaves):
    chips = leaves // 2
    fast = max(d for d in range(1, math.isqrt(chips) + 1) if chips % d == 0)
    return chips // fast, fast


def offset(value, step, count):
    if count & (count - 1):
        return lax.rem(value + step, count), lax.rem(value + count - step, count)
    bit = 1
    pair = value
    while bit < count:
        if step & bit:
            pair = pair + bit - 2 * bit * lax.rem(value // bit, 2)
        bit *= 2
    return pair, pair


def dot(left, right):
    return jnp.dot(left, right, preferred_element_type=F32)


def kernel(
    nr, nl,
    w_in, lr_in, lg_in, rf_in, ra_in, gf_in, ga_in,
    gr_out, gg_out, fr_out, fg_out,
    w, l, a, b, rt, rg, g, cb, rc, ys, ry, zs, rz, rx,
    ld, lb, out_sem, gz, gf, gy, gc, gx, gp, cs, yr, zr, xr, zn, yn, cn, xn,
):
    Z, Y = split_leaf(nl)
    obs, K = l.shape[1], l.shape[2]
    rows, half = K // nl, K // nr
    T = min(256, K)
    nb = obs // T
    r, leaf = lax.axis_index("region"), lax.axis_index("leaf")
    c, y, z = lax.rem(leaf, 2), lax.rem(leaf // 2, Y), leaf // (2 * Y)
    oc = 1 - c

    def at(zz, yy, cc):
        return (zz * Y + yy) * 2 + cc

    def zp(k):
        return offset(z, k, Z)[0]

    def zm(k):
        return offset(z, k, Z)[1]

    def yp(k):
        return offset(y, k, Y)[0]

    def ym(k):
        return offset(y, k, Y)[1]

    def rp(k):
        return lax.rem(r + k, nr)

    def rm(k):
        return lax.rem(r + nr - k, nr)

    def back(k, count):
        return count - k if count & (count - 1) else k

    def span(index, size):
        return pl.ds(pl.multiple_of(index * size, size), size)

    mine = span(leaf, rows)
    own = span(r, half)
    def copies(sem, *pairs):
        return [pltpu.make_async_copy(src, dst, sem) for src, dst in pairs]

    first = copies(ld.at[0], (gf_in.at[0], rg.at[0, mine]), (ga_in.at[0], rg.at[1, mine]))
    halves = copies(ld.at[1], (rf_in, rt.at[0, own]), (ra_in, rt.at[1, own]))
    bands = []
    for i in range(nb):
        band, left = pl.ds(i * T, T), pl.ds(0, (i + 1) * T)
        bands.append(copies(lb.at[i], (w_in.at[0, band, left], w.at[band, left]), (lr_in.at[0, band], l.at[0, band])))
    second = copies(ld.at[2], (lg_in.at[0], l.at[1]))
    for load in first + sum(bands, []) + halves + second:
        load.start()

    def taken(sem, count):
        whole = l.at[0, pl.ds(0, count)] if count <= obs else l.at[:, pl.ds(0, count // 2)]
        pltpu.make_async_copy(whole, whole, sem).wait()

    other = {"leaf": at(z, y, oc)}
    z_peers = [({"leaf": at(zp(k), y, c)}, zp(k) > z, zn.at[k - 1], zn.at[back(k, Z) - 1]) for k in range(1, Z)]
    y_peers = [({"leaf": at(z, yp(k), c)}, yp(k) > y, yn.at[k - 1], yn.at[back(k, Y) - 1]) for k in range(1, Y)]
    x_peers = [({"region": rp(k)}, rp(k) > r, xn.at[k - 1], xn.at[nr - k - 1]) for k in range(1, nr)]
    c_peers = [(other, oc > c, cn.at[0], cn.at[0])]
    peers = z_peers + y_peers + x_peers + c_peers

    barrier = pltpu.get_barrier_semaphore()
    for peer, later, _, _ in peers:
        @pl.when(later)
        def _():
            pl.semaphore_signal(barrier, inc=1, device_id=peer, device_id_type=MESH)
    pl.when(leaf + r > 0)(lambda: pl.semaphore_wait(barrier, z + y + r + c))
    for peer, later, _, theirs in peers:
        @pl.when(jnp.logical_not(later))
        def _():
            pl.semaphore_signal(theirs, inc=1, device_id=peer, device_id_type=MESH)

    sent = [0, 0]

    def plan(kind, src, dst, rsem, peer):
        sent[kind] += math.prod(src.shape) // K
        return pltpu.make_async_remote_copy(
            src_ref=src, dst_ref=dst, send_sem=out_sem.at[kind], recv_sem=rsem,
            device_id=peer, device_id_type=MESH,
        )

    def send(*args):
        plan(*args).start()

    def block(kz, ky, cc):
        return rg.at[:, span(at(zm(kz), ym(ky), cc), rows)]

    relayed = [k for k in range(3, Z, 2)] if Z & (Z - 1) == 0 else []

    def to_zs(ref, sems):
        return [
            plan(0, ref, ref, sems.at[k - 1], z_peers[k - 1][0]) if k not in relayed else None for k in range(1, Z)
        ]

    def relay(kz, ref, sems):
        if kz + 1 in relayed:
            plan(0, ref, ref, sems.at[kz], z_peers[0][0]).start()

    def to_ys(ref, kz):
        return [plan(0, ref, ref, gy.at[(k - 1) * Z + kz], y_peers[k - 1][0]) for k in range(1, Y)]

    def to_core(ref):
        return plan(0, ref, ref, gc.at[0], other)

    def from_z(kz):
        taken(gz.at[kz - 1], 2 * rows)
        relay(kz, block(kz, 0, c), gz)
        for copy in to_ys(block(kz, 0, c).at[1], kz) + [to_core(block(kz, 0, c))]:
            copy.start()

    def from_own_y(ky):
        taken(gy.at[(ky - 1) * Z], 2 * rows)
        for copy in to_zs(block(0, ky, c).at[0], gf.at[ky - 1]):
            if copy:
                copy.start()
        to_core(block(0, ky, c)).start()

    def from_y(kz, ky):
        taken(gy.at[(ky - 1) * Z + kz], rows)
        to_core(block(kz, ky, c).at[1]).start()

    def from_y_z(kz, ky):
        taken(gf.at[ky - 1, kz - 1], rows)
        relay(kz, block(kz, ky, c).at[0], gf.at[ky - 1])
        to_core(block(kz, ky, c).at[0]).start()

    to_z = to_zs(block(0, 0, c), gz)
    to_y = to_ys(block(0, 0, c), 0)
    to_c = [to_core(block(0, 0, c))]
    to_x = [plan(0, rt.at[c, own], rt.at[c, own], gx.at[k - 1], x_peers[k - 1][0]) for k in range(1, nr)]

    def open_early(group, copies):
        for (_, later, _, _), copy in zip(group, copies):
            if copy:
                pl.when(jnp.logical_not(later))(copy.start)

    def open_late(group, copies):
        for (_, later, sem, _), copy in zip(group, copies):
            @pl.when(later)
            def _():
                pl.semaphore_wait(sem, 1)
                if copy:
                    copy.start()

    scale = 1.0 / obs

    def a_band(p, i):
        a[p, pl.ds(i * T, T), :] = dot(
            w[pl.ds(i * T, T), pl.ds(0, (i + 1) * T)], l[p, pl.ds(0, (i + 1) * T), :]
        ).astype(BF16)

    step = max(T, 2 * Y * rows)
    per = step // (2 * Y * rows)
    parts = K // step

    def local_c(p):
        for i in range(parts):
            left = a[p, :, pl.ds(i * step, step)].T
            part = (dot(left, a[p]) * scale).astype(BF16)
            here = pl.ds(i * per, per)
            cb[p, here] = part.reshape(per, Y, 2, rows, K)
            send(1, cb.at[p, here, :, oc], rc.at[p, here], cs.at[p], other)

    def local_b(i):
        left = w[pl.ds(i * T, obs - i * T), pl.ds(i * T, T)].T
        for p in range(2):
            b[p, pl.ds(i * T, T), :] = dot(left, a[p, pl.ds(i * T, obs - i * T), :]).astype(BF16)

    far = range(Z - 1, -1, -1)

    def reduce_y(p):
        taken(cs.at[p], K // 2)
        for kz in far:
            zz = zp(kz)
            for k in range(1, Y):
                yy = yp(k)
                ys[p, k - 1, kz] = (cb[p, zz, yy, c].astype(F32) + rc[p, zz, yy].astype(F32)).astype(BF16)
                send(1, ys.at[p, k - 1, kz], ry.at[p, k - 1, kz], yr.at[p * Z + kz], {"leaf": at(z, yy, c)})

    def chip_sum(p, kz):
        zz = zp(kz)
        total = cb[p, zz, y, c].astype(F32) + rc[p, zz, y].astype(F32)
        if Y > 1:
            taken(yr.at[p * Z + kz], (Y - 1) * rows)
        for k in range(1, Y):
            total += ry[p, k - 1, kz].astype(F32)
        return total

    def reduce_z(p):
        for k in far[:-1]:
            zs[p, k - 1] = chip_sum(p, k).astype(BF16)
            send(1, zs.at[p, k - 1], rz.at[p, k - 1], zr.at[p], {"leaf": at(zp(k), y, c)})

    def finish_z(p):
        total = chip_sum(p, 0)
        if Z > 1:
            taken(zr.at[p], (Z - 1) * rows)
        for k in range(1, Z):
            total += rz[p, k - 1].astype(F32)
        return total

    def make_g(p, held):
        adjoint = held[1].astype(F32)
        g[p] = dot(held[0], (adjoint + adjoint.T).astype(BF16)).astype(BF16)

    def make_grad(p, out):
        for i in range(nb):
            part = pl.ds(i * T, T)
            out[0, part, :] = dot(b[p, part, :], g[p]).astype(BF16)

    taken(ld.at[0], 2 * rows)
    open_early(y_peers, to_y)
    open_early(z_peers, to_z)
    open_early(c_peers, to_c)
    for i in range(nb):
        taken(lb.at[i], (i + 1) * T * T // K + T)
        a_band(0, i)
    open_late(c_peers, to_c)
    open_late(y_peers, to_y)
    open_late(z_peers, to_z)
    local_c(0)
    taken(ld.at[1], 2 * half)
    open_early(x_peers, to_x)
    open_late(x_peers, to_x)
    taken(ld.at[2], obs)
    for i in range(nb):
        a_band(1, i)
    reduce_y(0)
    local_c(1)
    for ky in range(1, Y):
        from_own_y(ky)
    local_b(0)
    reduce_y(1)
    for k in range(1, max(Z, nb)):
        if k < Z and k not in relayed:
            from_z(k)
        if k < nb:
            local_b(k)
    reduce_z(0)
    for ky in range(1, Y):
        for k in range(1, Z):
            if k not in relayed:
                from_y_z(k, ky)
    for k in relayed:
        from_z(k)
    for k in range(1, nr):
        theirs = rt.at[c, span(rm(k), half)]
        taken(gx.at[k - 1], half)
        send(0, theirs, theirs, gp.at[0], other)
    if nr > 1:
        taken(gp.at[0], (nr - 1) * half)
    make_g(0, rt)
    reduce_z(1)
    make_grad(0, gr_out)
    rx[r] = finish_z(0).astype(BF16)
    for k in range(1, nr):
        send(1, rx.at[r], rx.at[r], xr.at[0], {"region": rp(k)})
    for ky in range(1, Y):
        for k in relayed:
            from_y_z(k, ky)
        for k in range(1, Z):
            from_y(k, ky)
    taken(gc.at[0], K)
    make_g(1, rg)
    make_grad(1, gg_out)
    fg_out[0] = dot(finish_z(1).astype(BF16), g[1])
    if nr > 1:
        taken(xr.at[0], (nr - 1) * rows)
    total = rx[0].astype(F32)
    for k in range(1, nr):
        total += rx[k].astype(F32)
    fr_out[...] = dot(total.astype(BF16), g[0])
    for kind in range(2):
        taken(out_sem.at[kind], sent[kind])


def store(*refs):
    held, target, store_sem = refs[:4], refs[4:8], refs[8]
    stores = [pltpu.make_async_copy(held[n], target[n], store_sem.at[n]) for n in range(4)]
    for save in stores:
        save.start()
    for save in stores:
        save.wait()


def solution(mesh):
    nr, nl = mesh.shape["region"], mesh.shape["leaf"]
    Z, Y = split_leaf(nl)

    def on_device(whiten, leaf_root, leaf_region, root_factor, root_adjoint, region_factor, region_adjoint):
        obs, K = leaf_root.shape[1], leaf_root.shape[2]
        rows = K // nl
        dma = lambda n: pltpu.SemaphoreType.DMA((max(n, 1),))
        flag = lambda n: pltpu.SemaphoreType.REGULAR((max(n, 1),))
        args = [pltpu.with_memory_space_constraint(x, pltpu.HBM) for x in (
            whiten, leaf_root, leaf_region, root_factor, root_adjoint, region_factor, region_adjoint)]
        held = pl.pallas_call(
            functools.partial(kernel, nr, nl),
            out_shape=(
                jax.ShapeDtypeStruct(leaf_root.shape, BF16),
                jax.ShapeDtypeStruct(leaf_region.shape, BF16),
                jax.ShapeDtypeStruct((rows, K), F32),
                jax.ShapeDtypeStruct((1, rows, K), F32),
            ),
            in_specs=[pl.BlockSpec(memory_space=pltpu.HBM)] * 7,
            out_specs=(pl.BlockSpec(memory_space=pltpu.VMEM),) * 4,
            scratch_shapes=[
                pltpu.VMEM((obs, obs), BF16),
                pltpu.VMEM((2, obs, K), BF16),
                pltpu.VMEM((2, obs, K), BF16),
                pltpu.VMEM((2, obs, K), BF16),
                pltpu.VMEM((2, K, K), BF16),
                pltpu.VMEM((2, K, K), BF16),
                pltpu.VMEM((2, K, K), BF16),
                pltpu.VMEM((2, Z, Y, 2, rows, K), BF16),
                pltpu.VMEM((2, Z, Y, rows, K), BF16),
                pltpu.VMEM((2, max(Y - 1, 1), Z, rows, K), BF16),
                pltpu.VMEM((2, max(Y - 1, 1), Z, rows, K), BF16),
                pltpu.VMEM((2, max(Z - 1, 1), rows, K), BF16),
                pltpu.VMEM((2, max(Z - 1, 1), rows, K), BF16),
                pltpu.VMEM((nr, rows, K), BF16),
                dma(3), dma(obs // min(256, K)), dma(2),
                dma(Z - 1), pltpu.SemaphoreType.DMA((max(Y - 1, 1), max(Z - 1, 1))), dma((Y - 1) * Z), dma(1), dma(nr - 1), dma(1), dma(2), dma(2 * Z), dma(2), dma(1),
                flag(Z - 1), flag(Y - 1), flag(1), flag(nr - 1),
            ],
            compiler_params=pltpu.CompilerParams(
                collective_id=0, has_side_effects=True, vmem_limit_bytes=40 << 20
            ),
            name="likelihood_backward",
        )(*args)
        return pl.pallas_call(
            store,
            out_shape=tuple(jax.ShapeDtypeStruct(x.shape, x.dtype) for x in held),
            in_specs=[pl.BlockSpec(memory_space=pltpu.VMEM)] * 4,
            out_specs=(pl.BlockSpec(memory_space=pltpu.HBM),) * 4,
            scratch_shapes=[dma(4)],
            compiler_params=pltpu.CompilerParams(vmem_limit_bytes=1 << 20),
            name="store_outputs",
        )(*held)

    return jax.shard_map(
        on_device,
        mesh=mesh,
        in_specs=(
            P(("region", "leaf"), None, None),
            P(("region", "leaf"), None, None),
            P(("region", "leaf"), None, None),
            P("region", None),
            P("region", None),
            P("region", "leaf", None),
            P("region", "leaf", None),
        ),
        out_specs=(
            P(("region", "leaf"), None, None),
            P(("region", "leaf"), None, None),
            P("leaf", None),
            P("region", "leaf", None),
        ),
        check_vma=False,
    )
```

```python
import functools
import math

import jax
import jax.numpy as jnp
from jax import lax
from jax.experimental import pallas as pl
from jax.experimental.pallas import tpu as pltpu
from jax.sharding import PartitionSpec as P

MESH = pl.DeviceIdType.MESH
F32, BF16 = jnp.float32, jnp.bfloat16


def split_leaf(leaves):
    chips = leaves // 2
    fast = max(d for d in range(1, math.isqrt(chips) + 1) if chips % d == 0)
    return chips // fast, fast


def offset(value, step, count):
    if count & (count - 1):
        return lax.rem(value + step, count), lax.rem(value + count - step, count)
    bit = 1
    pair = value
    while bit < count:
        if step & bit:
            pair = pair + bit - 2 * bit * lax.rem(value // bit, 2)
        bit *= 2
    return pair, pair


def dot(left, right):
    return jnp.dot(left, right, preferred_element_type=F32)


def kernel(
    nr, nl,
    w_in, lr_in, lg_in, rf_in, ra_in, gf_in, ga_in,
    gr_out, gg_out, fr_out, fg_out,
    w, l, a, b, rt, rg, g, cb, rc, ys, ry, zs, rz, rx,
    ld, lb, out_sem, gz, gf, gy, gc, gx, gp, cs, yr, zr, xr, zn, yn, cn, xn,
):
    Z, Y = split_leaf(nl)
    obs, K = l.shape[1], l.shape[2]
    rows, half = K // nl, K // nr
    T = min(256, K)
    nb = obs // T
    r, leaf = lax.axis_index("region"), lax.axis_index("leaf")
    c, y, z = lax.rem(leaf, 2), lax.rem(leaf // 2, Y), leaf // (2 * Y)
    oc = 1 - c

    def at(zz, yy, cc):
        return (zz * Y + yy) * 2 + cc

    def zp(k):
        return offset(z, k, Z)[0]

    def zm(k):
        return offset(z, k, Z)[1]

    def yp(k):
        return offset(y, k, Y)[0]

    def ym(k):
        return offset(y, k, Y)[1]

    def rp(k):
        return lax.rem(r + k, nr)

    def rm(k):
        return lax.rem(r + nr - k, nr)

    def back(k, count):
        return count - k if count & (count - 1) else k

    def span(index, size):
        return pl.ds(pl.multiple_of(index * size, size), size)

    mine = span(leaf, rows)
    own = span(r, half)
    def copies(sem, *pairs):
        return [pltpu.make_async_copy(src, dst, sem) for src, dst in pairs]

    first = copies(ld.at[0], (gf_in.at[0], rg.at[0, mine]), (ga_in.at[0], rg.at[1, mine]))
    halves = copies(ld.at[1], (rf_in, rt.at[0, own]), (ra_in, rt.at[1, own]))
    bands = []
    for i in range(nb):
        band, left = pl.ds(i * T, T), pl.ds(0, (i + 1) * T)
        bands.append(copies(lb.at[i], (w_in.at[0, band, left], w.at[band, left]), (lr_in.at[0, band], l.at[0, band])))
    second = copies(ld.at[2], (lg_in.at[0], l.at[1]))
    for load in first + sum(bands, []) + halves + second:
        load.start()

    def taken(sem, count):
        whole = l.at[0, pl.ds(0, count)] if count <= obs else l.at[:, pl.ds(0, count // 2)]
        pltpu.make_async_copy(whole, whole, sem).wait()

    other = {"leaf": at(z, y, oc)}
    z_peers = [({"leaf": at(zp(k), y, c)}, zp(k) > z, zn.at[k - 1], zn.at[back(k, Z) - 1]) for k in range(1, Z)]
    y_peers = [({"leaf": at(z, yp(k), c)}, yp(k) > y, yn.at[k - 1], yn.at[back(k, Y) - 1]) for k in range(1, Y)]
    x_peers = [({"region": rp(k)}, rp(k) > r, xn.at[k - 1], xn.at[nr - k - 1]) for k in range(1, nr)]
    c_peers = [(other, oc > c, cn.at[0], cn.at[0])]
    peers = z_peers + y_peers + x_peers + c_peers

    barrier = pltpu.get_barrier_semaphore()
    for peer, later, _, _ in peers:
        @pl.when(later)
        def _():
            pl.semaphore_signal(barrier, inc=1, device_id=peer, device_id_type=MESH)
    pl.when(leaf + r > 0)(lambda: pl.semaphore_wait(barrier, z + y + r + c))
    for peer, later, _, theirs in peers:
        @pl.when(jnp.logical_not(later))
        def _():
            pl.semaphore_signal(theirs, inc=1, device_id=peer, device_id_type=MESH)

    sent = [0, 0]

    def plan(kind, src, dst, rsem, peer):
        sent[kind] += math.prod(src.shape) // K
        return pltpu.make_async_remote_copy(
            src_ref=src, dst_ref=dst, send_sem=out_sem.at[kind], recv_sem=rsem,
            device_id=peer, device_id_type=MESH,
        )

    def send(*args):
        plan(*args).start()

    def block(kz, ky, cc):
        return rg.at[:, span(at(zm(kz), ym(ky), cc), rows)]

    relayed = [k for k in range(3, Z, 2)] if Z & (Z - 1) == 0 else []

    def to_zs(ref, sems):
        return [
            plan(0, ref, ref, sems.at[k - 1], z_peers[k - 1][0]) if k not in relayed else None for k in range(1, Z)
        ]

    def relay(kz, ref, sems):
        if kz + 1 in relayed:
            plan(0, ref, ref, sems.at[kz], z_peers[0][0]).start()

    def to_ys(ref, kz):
        return [plan(0, ref, ref, gy.at[(k - 1) * Z + kz], y_peers[k - 1][0]) for k in range(1, Y)]

    def to_core(ref):
        return plan(0, ref, ref, gc.at[0], other)

    def from_z(kz):
        taken(gz.at[kz - 1], 2 * rows)
        relay(kz, block(kz, 0, c), gz)
        held = block(kz, 0, c)
        for copy in to_ys(held if kz in relayed else held.at[1], kz) + [to_core(held)]:
            copy.start()

    def from_own_y(ky):
        taken(gy.at[(ky - 1) * Z], 2 * rows)
        for copy in to_zs(block(0, ky, c).at[0], gf.at[ky - 1]):
            if copy:
                copy.start()
        to_core(block(0, ky, c)).start()

    def from_y(kz, ky):
        held = block(kz, ky, c)
        taken(gy.at[(ky - 1) * Z + kz], 2 * rows if kz in relayed else rows)
        to_core(held if kz in relayed else held.at[1]).start()

    def from_y_z(kz, ky):
        taken(gf.at[ky - 1, kz - 1], rows)
        to_core(block(kz, ky, c).at[0]).start()

    to_z = to_zs(block(0, 0, c), gz)
    to_y = to_ys(block(0, 0, c), 0)
    to_c = [to_core(block(0, 0, c))]
    to_x = [plan(0, rt.at[c, own], rt.at[c, own], gx.at[k - 1], x_peers[k - 1][0]) for k in range(1, nr)]

    def open_early(group, copies):
        for (_, later, _, _), copy in zip(group, copies):
            if copy:
                pl.when(jnp.logical_not(later))(copy.start)

    def open_late(group, copies):
        for (_, later, sem, _), copy in zip(group, copies):
            @pl.when(later)
            def _():
                pl.semaphore_wait(sem, 1)
                if copy:
                    copy.start()

    scale = 1.0 / obs

    def a_band(p, i):
        a[p, pl.ds(i * T, T), :] = dot(
            w[pl.ds(i * T, T), pl.ds(0, (i + 1) * T)], l[p, pl.ds(0, (i + 1) * T), :]
        ).astype(BF16)

    step = max(T, 2 * Y * rows)
    per = step // (2 * Y * rows)
    parts = K // step

    def local_c(p):
        for i in range(parts):
            left = a[p, :, pl.ds(i * step, step)].T
            part = (dot(left, a[p]) * scale).astype(BF16)
            here = pl.ds(i * per, per)
            cb[p, here] = part.reshape(per, Y, 2, rows, K)
            send(1, cb.at[p, here, :, oc], rc.at[p, here], cs.at[p], other)

    def local_b(i):
        left = w[pl.ds(i * T, obs - i * T), pl.ds(i * T, T)].T
        for p in range(2):
            b[p, pl.ds(i * T, T), :] = dot(left, a[p, pl.ds(i * T, obs - i * T), :]).astype(BF16)

    far = range(Z - 1, -1, -1)

    def reduce_y(p):
        taken(cs.at[p], K // 2)
        for kz in far:
            zz = zp(kz)
            for k in range(1, Y):
                yy = yp(k)
                ys[p, k - 1, kz] = (cb[p, zz, yy, c].astype(F32) + rc[p, zz, yy].astype(F32)).astype(BF16)
                send(1, ys.at[p, k - 1, kz], ry.at[p, k - 1, kz], yr.at[p * Z + kz], {"leaf": at(z, yy, c)})

    def chip_sum(p, kz):
        zz = zp(kz)
        total = cb[p, zz, y, c].astype(F32) + rc[p, zz, y].astype(F32)
        if Y > 1:
            taken(yr.at[p * Z + kz], (Y - 1) * rows)
        for k in range(1, Y):
            total += ry[p, k - 1, kz].astype(F32)
        return total

    def reduce_z(p):
        for k in far[:-1]:
            zs[p, k - 1] = chip_sum(p, k).astype(BF16)
            send(1, zs.at[p, k - 1], rz.at[p, k - 1], zr.at[p], {"leaf": at(zp(k), y, c)})

    def finish_z(p):
        total = chip_sum(p, 0)
        if Z > 1:
            taken(zr.at[p], (Z - 1) * rows)
        for k in range(1, Z):
            total += rz[p, k - 1].astype(F32)
        return total

    def make_g(p, held):
        adjoint = held[1].astype(F32)
        g[p] = dot(held[0], (adjoint + adjoint.T).astype(BF16)).astype(BF16)

    def make_grad(p, out):
        for i in range(nb):
            part = pl.ds(i * T, T)
            out[0, part, :] = dot(b[p, part, :], g[p]).astype(BF16)

    taken(ld.at[0], 2 * rows)
    open_early(y_peers, to_y)
    open_early(z_peers, to_z)
    open_early(c_peers, to_c)
    for i in range(nb):
        taken(lb.at[i], (i + 1) * T * T // K + T)
        a_band(0, i)
    near = z >= Z // 2
    open_late(c_peers, to_c)
    taken(ld.at[1], 2 * half)
    open_early(x_peers, to_x)
    pl.when(near)(lambda: open_late(y_peers, to_y))
    pl.when(near)(lambda: open_late(z_peers, to_z))
    local_c(0)
    pl.when(jnp.logical_not(near))(lambda: open_late(y_peers, to_y))
    pl.when(jnp.logical_not(near))(lambda: open_late(z_peers, to_z))
    open_late(x_peers, to_x)
    taken(ld.at[2], obs)
    for i in range(nb):
        a_band(1, i)
    reduce_y(0)
    local_c(1)
    for ky in range(1, Y):
        from_own_y(ky)
    local_b(0)
    reduce_y(1)
    for k in range(1, max(Z, nb)):
        if k < Z and k not in relayed:
            from_z(k)
        if k < nb:
            local_b(k)
    reduce_z(0)
    for ky in range(1, Y):
        for k in range(1, Z):
            if k not in relayed:
                from_y_z(k, ky)
    for k in range(1, nr):
        theirs = rt.at[c, span(rm(k), half)]
        taken(gx.at[k - 1], half)
        send(0, theirs, theirs, gp.at[0], other)
    for k in relayed:
        from_z(k)
    reduce_z(1)
    if nr > 1:
        taken(gp.at[0], (nr - 1) * half)
    make_g(0, rt)
    make_grad(0, gr_out)
    rx[r] = finish_z(0).astype(BF16)
    for k in range(1, nr):
        send(1, rx.at[r], rx.at[r], xr.at[0], {"region": rp(k)})
    for ky in range(1, Y):
        for k in range(1, Z):
            from_y(k, ky)
    taken(gc.at[0], K)
    make_g(1, rg)
    make_grad(1, gg_out)
    fg_out[0] = dot(finish_z(1).astype(BF16), g[1])
    if nr > 1:
        taken(xr.at[0], (nr - 1) * rows)
    total = rx[0].astype(F32)
    for k in range(1, nr):
        total += rx[k].astype(F32)
    fr_out[...] = dot(total.astype(BF16), g[0])
    for kind in range(2):
        taken(out_sem.at[kind], sent[kind])


def store(*refs):
    held, target, store_sem = refs[:4], refs[4:8], refs[8]
    stores = [pltpu.make_async_copy(held[n], target[n], store_sem.at[n]) for n in range(4)]
    for save in stores:
        save.start()
    for save in stores:
        save.wait()


def solution(mesh):
    nr, nl = mesh.shape["region"], mesh.shape["leaf"]
    Z, Y = split_leaf(nl)

    def on_device(whiten, leaf_root, leaf_region, root_factor, root_adjoint, region_factor, region_adjoint):
        obs, K = leaf_root.shape[1], leaf_root.shape[2]
        rows = K // nl
        dma = lambda n: pltpu.SemaphoreType.DMA((max(n, 1),))
        flag = lambda n: pltpu.SemaphoreType.REGULAR((max(n, 1),))
        args = [pltpu.with_memory_space_constraint(x, pltpu.HBM) for x in (
            whiten, leaf_root, leaf_region, root_factor, root_adjoint, region_factor, region_adjoint)]
        held = pl.pallas_call(
            functools.partial(kernel, nr, nl),
            out_shape=(
                jax.ShapeDtypeStruct(leaf_root.shape, BF16),
                jax.ShapeDtypeStruct(leaf_region.shape, BF16),
                jax.ShapeDtypeStruct((rows, K), F32),
                jax.ShapeDtypeStruct((1, rows, K), F32),
            ),
            in_specs=[pl.BlockSpec(memory_space=pltpu.HBM)] * 7,
            out_specs=(pl.BlockSpec(memory_space=pltpu.VMEM),) * 4,
            scratch_shapes=[
                pltpu.VMEM((obs, obs), BF16),
                pltpu.VMEM((2, obs, K), BF16),
                pltpu.VMEM((2, obs, K), BF16),
                pltpu.VMEM((2, obs, K), BF16),
                pltpu.VMEM((2, K, K), BF16),
                pltpu.VMEM((2, K, K), BF16),
                pltpu.VMEM((2, K, K), BF16),
                pltpu.VMEM((2, Z, Y, 2, rows, K), BF16),
                pltpu.VMEM((2, Z, Y, rows, K), BF16),
                pltpu.VMEM((2, max(Y - 1, 1), Z, rows, K), BF16),
                pltpu.VMEM((2, max(Y - 1, 1), Z, rows, K), BF16),
                pltpu.VMEM((2, max(Z - 1, 1), rows, K), BF16),
                pltpu.VMEM((2, max(Z - 1, 1), rows, K), BF16),
                pltpu.VMEM((nr, rows, K), BF16),
                dma(3), dma(obs // min(256, K)), dma(2),
                dma(Z - 1), pltpu.SemaphoreType.DMA((max(Y - 1, 1), max(Z - 1, 1))), dma((Y - 1) * Z), dma(1), dma(nr - 1), dma(1), dma(2), dma(2 * Z), dma(2), dma(1),
                flag(Z - 1), flag(Y - 1), flag(1), flag(nr - 1),
            ],
            compiler_params=pltpu.CompilerParams(
                collective_id=0, has_side_effects=True, vmem_limit_bytes=40 << 20
            ),
            name="likelihood_backward",
        )(*args)
        return pl.pallas_call(
            store,
            out_shape=tuple(jax.ShapeDtypeStruct(x.shape, x.dtype) for x in held),
            in_specs=[pl.BlockSpec(memory_space=pltpu.VMEM)] * 4,
            out_specs=(pl.BlockSpec(memory_space=pltpu.HBM),) * 4,
            scratch_shapes=[dma(4)],
            compiler_params=pltpu.CompilerParams(vmem_limit_bytes=1 << 20),
            name="store_outputs",
        )(*held)

    return jax.shard_map(
        on_device,
        mesh=mesh,
        in_specs=(
            P(("region", "leaf"), None, None),
            P(("region", "leaf"), None, None),
            P(("region", "leaf"), None, None),
            P("region", None),
            P("region", None),
            P("region", "leaf", None),
            P("region", "leaf", None),
        ),
        out_specs=(
            P(("region", "leaf"), None, None),
            P(("region", "leaf"), None, None),
            P("leaf", None),
            P("region", "leaf", None),
        ),
        check_vma=False,
    )
```

```python
import functools
import math

import jax
import jax.numpy as jnp
from jax import lax
from jax.experimental import pallas as pl
from jax.experimental.pallas import tpu as pltpu
from jax.sharding import PartitionSpec as P

MESH = pl.DeviceIdType.MESH
F32, BF16 = jnp.float32, jnp.bfloat16


def split_leaf(leaves):
    chips = leaves // 2
    fast = max(d for d in range(1, math.isqrt(chips) + 1) if chips % d == 0)
    return chips // fast, fast


def offset(value, step, count):
    if count & (count - 1):
        return lax.rem(value + step, count), lax.rem(value + count - step, count)
    bit = 1
    pair = value
    while bit < count:
        if step & bit:
            pair = pair + bit - 2 * bit * lax.rem(value // bit, 2)
        bit *= 2
    return pair, pair


def dot(left, right):
    return jnp.dot(left, right, preferred_element_type=F32)


def kernel(
    nr, nl,
    w_in, lr_in, lg_in, rf_in, ra_in, gf_in, ga_in,
    gr_out, gg_out, fr_out, fg_out,
    w, l, a, b, rt, rg, g, cb, rc, ys, ry, zs, rz, rx,
    ld, lb, out_sem, gz, gf, gy, gc, gx, gp, cs, yr, zr, xr, zn, yn, cn, xn,
):
    Z, Y = split_leaf(nl)
    obs, K = l.shape[1], l.shape[2]
    rows, half = K // nl, K // nr
    T = min(256, K)
    nb = obs // T
    r, leaf = lax.axis_index("region"), lax.axis_index("leaf")
    c, y, z = lax.rem(leaf, 2), lax.rem(leaf // 2, Y), leaf // (2 * Y)
    oc = 1 - c

    def at(zz, yy, cc):
        return (zz * Y + yy) * 2 + cc

    def zp(k):
        return offset(z, k, Z)[0]

    def zm(k):
        return offset(z, k, Z)[1]

    def yp(k):
        return offset(y, k, Y)[0]

    def ym(k):
        return offset(y, k, Y)[1]

    def rp(k):
        return lax.rem(r + k, nr)

    def rm(k):
        return lax.rem(r + nr - k, nr)

    def back(k, count):
        return count - k if count & (count - 1) else k

    def span(index, size):
        return pl.ds(pl.multiple_of(index * size, size), size)

    mine = span(leaf, rows)
    own = span(r, half)
    def copies(sem, *pairs):
        return [pltpu.make_async_copy(src, dst, sem) for src, dst in pairs]

    first = copies(ld.at[0], (gf_in.at[0], rg.at[0, mine]), (ga_in.at[0], rg.at[1, mine]))
    halves = copies(ld.at[1], (rf_in, rt.at[0, own]), (ra_in, rt.at[1, own]))
    bands = []
    for i in range(nb):
        band, left = pl.ds(i * T, T), pl.ds(0, (i + 1) * T)
        bands.append(copies(lb.at[i], (w_in.at[0, band, left], w.at[band, left]), (lr_in.at[0, band], l.at[0, band])))
    second = copies(ld.at[2], (lg_in.at[0], l.at[1]))
    for load in first + sum(bands, []) + halves + second:
        load.start()

    def taken(sem, count):
        whole = l.at[0, pl.ds(0, count)] if count <= obs else l.at[:, pl.ds(0, count // 2)]
        pltpu.make_async_copy(whole, whole, sem).wait()

    other = {"leaf": at(z, y, oc)}
    z_peers = [({"leaf": at(zp(k), y, c)}, zp(k) > z, zn.at[k - 1], zn.at[back(k, Z) - 1]) for k in range(1, Z)]
    y_peers = [({"leaf": at(z, yp(k), c)}, yp(k) > y, yn.at[k - 1], yn.at[back(k, Y) - 1]) for k in range(1, Y)]
    x_peers = [({"region": rp(k)}, rp(k) > r, xn.at[k - 1], xn.at[nr - k - 1]) for k in range(1, nr)]
    c_peers = [(other, oc > c, cn.at[0], cn.at[0])]
    peers = z_peers + y_peers + x_peers + c_peers

    barrier = pltpu.get_barrier_semaphore()
    for peer, later, _, _ in peers:
        @pl.when(later)
        def _():
            pl.semaphore_signal(barrier, inc=1, device_id=peer, device_id_type=MESH)
    pl.when(leaf + r > 0)(lambda: pl.semaphore_wait(barrier, z + y + r + c))
    for peer, later, _, theirs in peers:
        @pl.when(jnp.logical_not(later))
        def _():
            pl.semaphore_signal(theirs, inc=1, device_id=peer, device_id_type=MESH)

    sent = [0, 0]

    def plan(kind, src, dst, rsem, peer):
        sent[kind] += math.prod(src.shape) // K
        return pltpu.make_async_remote_copy(
            src_ref=src, dst_ref=dst, send_sem=out_sem.at[kind], recv_sem=rsem,
            device_id=peer, device_id_type=MESH,
        )

    def send(*args):
        plan(*args).start()

    def block(kz, ky, cc):
        return rg.at[:, span(at(zm(kz), ym(ky), cc), rows)]

    relayed = [k for k in range(3, Z, 2)] if Z & (Z - 1) == 0 else []

    def to_zs(ref, sems):
        return [
            plan(0, ref, ref, sems.at[k - 1], z_peers[k - 1][0]) if k not in relayed else None for k in range(1, Z)
        ]

    def relay(kz, ref, sems):
        if kz + 1 in relayed:
            plan(0, ref, ref, sems.at[kz], z_peers[0][0]).start()

    def to_ys(ref, kz):
        return [plan(0, ref, ref, gy.at[(k - 1) * Z + kz], y_peers[k - 1][0]) for k in range(1, Y)]

    def to_core(ref):
        return plan(0, ref, ref, gc.at[0], other)

    def from_z(kz):
        taken(gz.at[kz - 1], 2 * rows)
        relay(kz, block(kz, 0, c), gz)
        held = block(kz, 0, c)
        for copy in to_ys(held if kz in relayed else held.at[1], kz) + [to_core(held)]:
            copy.start()

    def from_own_y(ky):
        taken(gy.at[(ky - 1) * Z], 2 * rows)
        for copy in to_zs(block(0, ky, c).at[0], gf.at[ky - 1]):
            if copy:
                copy.start()
        to_core(block(0, ky, c)).start()

    def from_y(kz, ky):
        held = block(kz, ky, c)
        taken(gy.at[(ky - 1) * Z + kz], 2 * rows if kz in relayed else rows)
        to_core(held if kz in relayed else held.at[1]).start()

    def from_y_z(kz, ky):
        taken(gf.at[ky - 1, kz - 1], rows)
        to_core(block(kz, ky, c).at[0]).start()

    to_z = to_zs(block(0, 0, c), gz)
    to_y = to_ys(block(0, 0, c), 0)
    to_c = [to_core(block(0, 0, c))]
    to_x = [plan(0, rt.at[c, own], rt.at[c, own], gx.at[k - 1], x_peers[k - 1][0]) for k in range(1, nr)]

    def open_early(group, copies):
        for (_, later, _, _), copy in zip(group, copies):
            if copy:
                pl.when(jnp.logical_not(later))(copy.start)

    def open_late(group, copies):
        for (_, later, sem, _), copy in zip(group, copies):
            @pl.when(later)
            def _():
                pl.semaphore_wait(sem, 1)
                if copy:
                    copy.start()

    scale = 1.0 / obs

    def a_band(p, i):
        a[p, pl.ds(i * T, T), :] = dot(
            w[pl.ds(i * T, T), pl.ds(0, (i + 1) * T)], l[p, pl.ds(0, (i + 1) * T), :]
        ).astype(BF16)

    step = max(T, 2 * Y * rows)
    per = step // (2 * Y * rows)
    parts = K // step

    def local_c(p):
        for i in range(parts):
            left = a[p, :, pl.ds(i * step, step)].T
            part = (dot(left, a[p]) * scale).astype(BF16)
            here = pl.ds(i * per, per)
            cb[p, here] = part.reshape(per, Y, 2, rows, K)
            send(1, cb.at[p, here, :, oc], rc.at[p, here], cs.at[p], other)

    def local_b(i):
        left = w[pl.ds(i * T, obs - i * T), pl.ds(i * T, T)].T
        for p in range(2):
            b[p, pl.ds(i * T, T), :] = dot(left, a[p, pl.ds(i * T, obs - i * T), :]).astype(BF16)

    far = range(Z - 1, -1, -1)

    def reduce_y(p):
        taken(cs.at[p], K // 2)
        for kz in far:
            zz = zp(kz)
            for k in range(1, Y):
                yy = yp(k)
                ys[p, k - 1, kz] = (cb[p, zz, yy, c].astype(F32) + rc[p, zz, yy].astype(F32)).astype(BF16)
                send(1, ys.at[p, k - 1, kz], ry.at[p, k - 1, kz], yr.at[p * Z + kz], {"leaf": at(z, yy, c)})

    def chip_sum(p, kz):
        zz = zp(kz)
        total = cb[p, zz, y, c].astype(F32) + rc[p, zz, y].astype(F32)
        if Y > 1:
            taken(yr.at[p * Z + kz], (Y - 1) * rows)
        for k in range(1, Y):
            total += ry[p, k - 1, kz].astype(F32)
        return total

    def reduce_z(p, ks=None):
        for k in ks or far[:-1]:
            zs[p, k - 1] = chip_sum(p, k).astype(BF16)
            send(1, zs.at[p, k - 1], rz.at[p, k - 1], zr.at[p], {"leaf": at(zp(k), y, c)})

    def finish_z(p):
        total = chip_sum(p, 0)
        if Z > 1:
            taken(zr.at[p], (Z - 1) * rows)
        for k in range(1, Z):
            total += rz[p, k - 1].astype(F32)
        return total

    def make_g(p, held):
        adjoint = held[1].astype(F32)
        g[p] = dot(held[0], (adjoint + adjoint.T).astype(BF16)).astype(BF16)

    def make_grad(p, out):
        for i in range(nb):
            part = pl.ds(i * T, T)
            out[0, part, :] = dot(b[p, part, :], g[p]).astype(BF16)

    taken(ld.at[0], 2 * rows)
    open_early(y_peers, to_y)
    open_early(z_peers, to_z)
    open_early(c_peers, to_c)
    for i in range(nb):
        taken(lb.at[i], (i + 1) * T * T // K + T)
        a_band(0, i)
    near = z >= Z // 2
    open_late(c_peers, to_c)
    taken(ld.at[1], 2 * half)
    open_early(x_peers, to_x)
    pl.when(near)(lambda: open_late(y_peers, to_y))
    pl.when(near)(lambda: open_late(z_peers, to_z))
    local_c(0)
    pl.when(jnp.logical_not(near))(lambda: open_late(y_peers, to_y))
    pl.when(jnp.logical_not(near))(lambda: open_late(z_peers, to_z))
    open_late(x_peers, to_x)
    taken(ld.at[2], obs)
    for i in range(nb):
        a_band(1, i)
    reduce_y(0)
    local_c(1)
    for ky in range(1, Y):
        from_own_y(ky)
    local_b(0)
    reduce_y(1)
    for k in relayed:
        from_z(k - 1)
    for k in range(1, max(Z, nb)):
        if k < Z and k not in relayed and k + 1 not in relayed:
            from_z(k)
        if k < nb - 1:
            local_b(k)
    reduce_z(0)
    local_b(nb - 1)
    for ky in range(1, Y):
        for k in range(1, Z):
            if k not in relayed:
                from_y_z(k, ky)
    for k in range(1, nr):
        theirs = rt.at[c, span(rm(k), half)]
        taken(gx.at[k - 1], half)
        send(0, theirs, theirs, gp.at[0], other)
    reduce_z(1, far[:1])
    for k in relayed:
        from_z(k)
    reduce_z(1, far[1:-1])
    if nr > 1:
        taken(gp.at[0], (nr - 1) * half)
    make_g(0, rt)
    make_grad(0, gr_out)
    rx[r] = finish_z(0).astype(BF16)
    for k in range(1, nr):
        send(1, rx.at[r], rx.at[r], xr.at[0], {"region": rp(k)})
    for ky in range(1, Y):
        for k in range(1, Z):
            from_y(k, ky)
    taken(gc.at[0], K)
    make_g(1, rg)
    make_grad(1, gg_out)
    fg_out[0] = dot(finish_z(1).astype(BF16), g[1])
    if nr > 1:
        taken(xr.at[0], (nr - 1) * rows)
    total = rx[0].astype(F32)
    for k in range(1, nr):
        total += rx[k].astype(F32)
    fr_out[...] = dot(total.astype(BF16), g[0])
    for kind in range(2):
        taken(out_sem.at[kind], sent[kind])


def store(*refs):
    held, target, store_sem = refs[:4], refs[4:8], refs[8]
    stores = [pltpu.make_async_copy(held[n], target[n], store_sem.at[n]) for n in range(4)]
    for save in stores:
        save.start()
    for save in stores:
        save.wait()


def solution(mesh):
    nr, nl = mesh.shape["region"], mesh.shape["leaf"]
    Z, Y = split_leaf(nl)

    def on_device(whiten, leaf_root, leaf_region, root_factor, root_adjoint, region_factor, region_adjoint):
        obs, K = leaf_root.shape[1], leaf_root.shape[2]
        rows = K // nl
        dma = lambda n: pltpu.SemaphoreType.DMA((max(n, 1),))
        flag = lambda n: pltpu.SemaphoreType.REGULAR((max(n, 1),))
        args = [pltpu.with_memory_space_constraint(x, pltpu.HBM) for x in (
            whiten, leaf_root, leaf_region, root_factor, root_adjoint, region_factor, region_adjoint)]
        held = pl.pallas_call(
            functools.partial(kernel, nr, nl),
            out_shape=(
                jax.ShapeDtypeStruct(leaf_root.shape, BF16),
                jax.ShapeDtypeStruct(leaf_region.shape, BF16),
                jax.ShapeDtypeStruct((rows, K), F32),
                jax.ShapeDtypeStruct((1, rows, K), F32),
            ),
            in_specs=[pl.BlockSpec(memory_space=pltpu.HBM)] * 7,
            out_specs=(pl.BlockSpec(memory_space=pltpu.VMEM),) * 4,
            scratch_shapes=[
                pltpu.VMEM((obs, obs), BF16),
                pltpu.VMEM((2, obs, K), BF16),
                pltpu.VMEM((2, obs, K), BF16),
                pltpu.VMEM((2, obs, K), BF16),
                pltpu.VMEM((2, K, K), BF16),
                pltpu.VMEM((2, K, K), BF16),
                pltpu.VMEM((2, K, K), BF16),
                pltpu.VMEM((2, Z, Y, 2, rows, K), BF16),
                pltpu.VMEM((2, Z, Y, rows, K), BF16),
                pltpu.VMEM((2, max(Y - 1, 1), Z, rows, K), BF16),
                pltpu.VMEM((2, max(Y - 1, 1), Z, rows, K), BF16),
                pltpu.VMEM((2, max(Z - 1, 1), rows, K), BF16),
                pltpu.VMEM((2, max(Z - 1, 1), rows, K), BF16),
                pltpu.VMEM((nr, rows, K), BF16),
                dma(3), dma(obs // min(256, K)), dma(2),
                dma(Z - 1), pltpu.SemaphoreType.DMA((max(Y - 1, 1), max(Z - 1, 1))), dma((Y - 1) * Z), dma(1), dma(nr - 1), dma(1), dma(2), dma(2 * Z), dma(2), dma(1),
                flag(Z - 1), flag(Y - 1), flag(1), flag(nr - 1),
            ],
            compiler_params=pltpu.CompilerParams(
                collective_id=0, has_side_effects=True, vmem_limit_bytes=40 << 20
            ),
            name="likelihood_backward",
        )(*args)
        return pl.pallas_call(
            store,
            out_shape=tuple(jax.ShapeDtypeStruct(x.shape, x.dtype) for x in held),
            in_specs=[pl.BlockSpec(memory_space=pltpu.VMEM)] * 4,
            out_specs=(pl.BlockSpec(memory_space=pltpu.HBM),) * 4,
            scratch_shapes=[dma(4)],
            compiler_params=pltpu.CompilerParams(vmem_limit_bytes=1 << 20),
            name="store_outputs",
        )(*held)

    return jax.shard_map(
        on_device,
        mesh=mesh,
        in_specs=(
            P(("region", "leaf"), None, None),
            P(("region", "leaf"), None, None),
            P(("region", "leaf"), None, None),
            P("region", None),
            P("region", None),
            P("region", "leaf", None),
            P("region", "leaf", None),
        ),
        out_specs=(
            P(("region", "leaf"), None, None),
            P(("region", "leaf"), None, None),
            P("leaf", None),
            P("region", "leaf", None),
        ),
        check_vma=False,
    )
```

```python
import functools
import math

import jax
import jax.numpy as jnp
from jax import lax
from jax.experimental import pallas as pl
from jax.experimental.pallas import tpu as pltpu
from jax.sharding import PartitionSpec as P

MESH = pl.DeviceIdType.MESH
F32, BF16 = jnp.float32, jnp.bfloat16


def split_leaf(leaves):
    chips = leaves // 2
    fast = max(d for d in range(1, math.isqrt(chips) + 1) if chips % d == 0)
    return chips // fast, fast


def offset(value, step, count):
    if count & (count - 1):
        return lax.rem(value + step, count), lax.rem(value + count - step, count)
    bit = 1
    pair = value
    while bit < count:
        if step & bit:
            pair = pair + bit - 2 * bit * lax.rem(value // bit, 2)
        bit *= 2
    return pair, pair


def dot(left, right):
    return jnp.dot(left, right, preferred_element_type=F32)


def kernel(
    nr, nl,
    w_in, lr_in, lg_in, rf_in, ra_in, gf_in, ga_in,
    gr_out, gg_out, fr_out, fg_out,
    w, l, a, b, rt, rg, g, cb, rc, ys, ry, zs, rz, rx,
    ld, lb, out_sem, gz, gf, gy, gc, gx, gp, cs, yr, zr, xr, zn, yn, cn, xn,
):
    Z, Y = split_leaf(nl)
    obs, K = l.shape[1], l.shape[2]
    rows, half = K // nl, K // nr
    T = min(256, K)
    nb = obs // T
    r, leaf = lax.axis_index("region"), lax.axis_index("leaf")
    c, y, z = lax.rem(leaf, 2), lax.rem(leaf // 2, Y), leaf // (2 * Y)
    oc = 1 - c

    def at(zz, yy, cc):
        return (zz * Y + yy) * 2 + cc

    def zp(k):
        return offset(z, k, Z)[0]

    def zm(k):
        return offset(z, k, Z)[1]

    def yp(k):
        return offset(y, k, Y)[0]

    def ym(k):
        return offset(y, k, Y)[1]

    def rp(k):
        return lax.rem(r + k, nr)

    def rm(k):
        return lax.rem(r + nr - k, nr)

    def back(k, count):
        return count - k if count & (count - 1) else k

    def span(index, size):
        return pl.ds(pl.multiple_of(index * size, size), size)

    mine = span(leaf, rows)
    own = span(r, half)
    def copies(sem, *pairs):
        return [pltpu.make_async_copy(src, dst, sem) for src, dst in pairs]

    first = copies(ld.at[0], (gf_in.at[0], rg.at[0, mine]), (ga_in.at[0], rg.at[1, mine]))
    halves = copies(ld.at[1], (rf_in, rt.at[0, own]), (ra_in, rt.at[1, own]))
    bands = []
    for i in range(nb):
        band, left = pl.ds(i * T, T), pl.ds(0, (i + 1) * T)
        bands.append(copies(lb.at[i], (w_in.at[0, band, left], w.at[band, left]), (lr_in.at[0, band], l.at[0, band])))
    second = copies(ld.at[2], (lg_in.at[0], l.at[1]))
    for load in first + sum(bands, []) + halves + second:
        load.start()

    def taken(sem, count):
        whole = l.at[0, pl.ds(0, count)] if count <= obs else l.at[:, pl.ds(0, count // 2)]
        pltpu.make_async_copy(whole, whole, sem).wait()

    other = {"leaf": at(z, y, oc)}
    z_peers = [({"leaf": at(zp(k), y, c)}, zp(k) > z, zn.at[k - 1], zn.at[back(k, Z) - 1]) for k in range(1, Z)]
    y_peers = [({"leaf": at(z, yp(k), c)}, yp(k) > y, yn.at[k - 1], yn.at[back(k, Y) - 1]) for k in range(1, Y)]
    x_peers = [({"region": rp(k)}, rp(k) > r, xn.at[k - 1], xn.at[nr - k - 1]) for k in range(1, nr)]
    c_peers = [(other, oc > c, cn.at[0], cn.at[0])]
    peers = z_peers + y_peers + x_peers + c_peers

    barrier = pltpu.get_barrier_semaphore()
    for peer, later, _, _ in peers:
        @pl.when(later)
        def _():
            pl.semaphore_signal(barrier, inc=1, device_id=peer, device_id_type=MESH)
    pl.when(leaf + r > 0)(lambda: pl.semaphore_wait(barrier, z + y + r + c))
    for peer, later, _, theirs in peers:
        @pl.when(jnp.logical_not(later))
        def _():
            pl.semaphore_signal(theirs, inc=1, device_id=peer, device_id_type=MESH)

    sent = [0, 0]

    def plan(kind, src, dst, rsem, peer):
        sent[kind] += math.prod(src.shape) // K
        return pltpu.make_async_remote_copy(
            src_ref=src, dst_ref=dst, send_sem=out_sem.at[kind], recv_sem=rsem,
            device_id=peer, device_id_type=MESH,
        )

    def send(*args):
        plan(*args).start()

    def block(kz, ky, cc):
        return rg.at[:, span(at(zm(kz), ym(ky), cc), rows)]

    relayed = [k for k in range(3, Z, 2)] if Z & (Z - 1) == 0 else []

    def to_zs(ref, sems):
        return [
            plan(0, ref, ref, sems.at[k - 1], z_peers[k - 1][0]) if k not in relayed else None for k in range(1, Z)
        ]

    def relay(kz, ref, sems):
        if kz + 1 in relayed:
            plan(0, ref, ref, sems.at[kz], z_peers[0][0]).start()

    def to_ys(ref, kz):
        return [plan(0, ref, ref, gy.at[(k - 1) * Z + kz], y_peers[k - 1][0]) for k in range(1, Y)]

    def to_core(ref):
        return plan(0, ref, ref, gc.at[0], other)

    def from_z(kz):
        taken(gz.at[kz - 1], 2 * rows)
        relay(kz, block(kz, 0, c), gz)
        held = block(kz, 0, c)
        for copy in to_ys(held if kz in relayed else held.at[1], kz) + [to_core(held)]:
            copy.start()

    def from_own_y(ky):
        taken(gy.at[(ky - 1) * Z], 2 * rows)
        for copy in to_zs(block(0, ky, c).at[0], gf.at[ky - 1]):
            if copy:
                copy.start()
        to_core(block(0, ky, c)).start()

    def from_y(kz, ky):
        held = block(kz, ky, c)
        taken(gy.at[(ky - 1) * Z + kz], 2 * rows if kz in relayed else rows)
        to_core(held if kz in relayed else held.at[1]).start()

    def from_y_z(kz, ky):
        taken(gf.at[ky - 1, kz - 1], rows)
        to_core(block(kz, ky, c).at[0]).start()

    to_z = to_zs(block(0, 0, c), gz)
    to_y = to_ys(block(0, 0, c), 0)
    to_c = [to_core(block(0, 0, c))]
    to_x = [plan(0, rt.at[c, own], rt.at[c, own], gx.at[k - 1], x_peers[k - 1][0]) for k in range(1, nr)]

    def open_early(group, copies):
        for (_, later, _, _), copy in zip(group, copies):
            if copy:
                pl.when(jnp.logical_not(later))(copy.start)

    def open_late(group, copies):
        for (_, later, sem, _), copy in zip(group, copies):
            @pl.when(later)
            def _():
                pl.semaphore_wait(sem, 1)
                if copy:
                    copy.start()

    scale = 1.0 / obs

    def a_band(p, i):
        a[p, pl.ds(i * T, T), :] = dot(
            w[pl.ds(i * T, T), pl.ds(0, (i + 1) * T)], l[p, pl.ds(0, (i + 1) * T), :]
        ).astype(BF16)

    step = max(T, 2 * Y * rows)
    per = step // (2 * Y * rows)
    parts = K // step

    def local_c(p):
        for i in range(parts):
            left = a[p, :, pl.ds(i * step, step)].T
            part = (dot(left, a[p]) * scale).astype(BF16)
            here = pl.ds(i * per, per)
            cb[p, here] = part.reshape(per, Y, 2, rows, K)
            send(1, cb.at[p, here, :, oc], rc.at[p, here], cs.at[p], other)

    def local_b(i):
        left = w[pl.ds(i * T, obs - i * T), pl.ds(i * T, T)].T
        for p in range(2):
            b[p, pl.ds(i * T, T), :] = dot(left, a[p, pl.ds(i * T, obs - i * T), :]).astype(BF16)

    far = range(Z - 1, -1, -1)

    def reduce_y(p):
        taken(cs.at[p], K // 2)
        for kz in far:
            zz = zp(kz)
            for k in range(1, Y):
                yy = yp(k)
                ys[p, k - 1, kz] = (cb[p, zz, yy, c].astype(F32) + rc[p, zz, yy].astype(F32)).astype(BF16)
                send(1, ys.at[p, k - 1, kz], ry.at[p, k - 1, kz], yr.at[p * Z + kz], {"leaf": at(z, yy, c)})

    def chip_sum(p, kz):
        zz = zp(kz)
        total = cb[p, zz, y, c].astype(F32) + rc[p, zz, y].astype(F32)
        if Y > 1:
            taken(yr.at[p * Z + kz], (Y - 1) * rows)
        for k in range(1, Y):
            total += ry[p, k - 1, kz].astype(F32)
        return total

    def reduce_z(p, ks=None):
        for k in ks or far[:-1]:
            zs[p, k - 1] = chip_sum(p, k).astype(BF16)
            send(1, zs.at[p, k - 1], rz.at[p, k - 1], zr.at[p], {"leaf": at(zp(k), y, c)})

    def finish_z(p):
        total = chip_sum(p, 0)
        if Z > 1:
            taken(zr.at[p], (Z - 1) * rows)
        for k in range(1, Z):
            total += rz[p, k - 1].astype(F32)
        return total

    def make_g(p, held):
        adjoint = held[1].astype(F32)
        g[p] = dot(held[0], (adjoint + adjoint.T).astype(BF16)).astype(BF16)

    def make_grad(p, out):
        for i in range(nb):
            part = pl.ds(i * T, T)
            out[0, part, :] = dot(b[p, part, :], g[p]).astype(BF16)

    taken(ld.at[0], 2 * rows)
    open_early(y_peers, to_y)
    open_early(z_peers, to_z)
    open_early(c_peers, to_c)
    for i in range(nb):
        taken(lb.at[i], (i + 1) * T * T // K + T)
        a_band(0, i)
    near = z >= Z // 2
    open_late(c_peers, to_c)
    taken(ld.at[1], 2 * half)
    open_early(x_peers, to_x)
    pl.when(near)(lambda: open_late(y_peers, to_y))
    pl.when(near)(lambda: open_late(z_peers, to_z))
    local_c(0)
    pl.when(jnp.logical_not(near))(lambda: open_late(y_peers, to_y))
    pl.when(jnp.logical_not(near))(lambda: open_late(z_peers, to_z))
    open_late(x_peers, to_x)
    taken(ld.at[2], obs)
    for i in range(nb):
        a_band(1, i)
    reduce_y(0)
    local_c(1)
    for ky in range(1, Y):
        from_own_y(ky)
    local_b(0)
    reduce_y(1)
    for k in relayed:
        from_z(k - 1)
    for k in range(1, max(Z, nb)):
        if k < Z and k not in relayed and k + 1 not in relayed:
            from_z(k)
        if k < nb - 1:
            local_b(k)
    reduce_z(0)
    for ky in range(1, Y):
        for k in range(1, Z):
            if k not in relayed:
                from_y_z(k, ky)
    for k in range(1, nr):
        theirs = rt.at[c, span(rm(k), half)]
        taken(gx.at[k - 1], half)
        send(0, theirs, theirs, gp.at[0], other)
    reduce_z(1, far[:1])
    local_b(nb - 1)
    for k in relayed:
        from_z(k)
    reduce_z(1, far[1:-1])
    if nr > 1:
        taken(gp.at[0], (nr - 1) * half)
    make_g(0, rt)
    make_grad(0, gr_out)
    rx[r] = finish_z(0).astype(BF16)
    for k in range(1, nr):
        send(1, rx.at[r], rx.at[r], xr.at[0], {"region": rp(k)})
    for ky in range(1, Y):
        for k in range(1, Z):
            from_y(k, ky)
    taken(gc.at[0], K)
    make_g(1, rg)
    make_grad(1, gg_out)
    fg_out[0] = dot(finish_z(1).astype(BF16), g[1])
    if nr > 1:
        taken(xr.at[0], (nr - 1) * rows)
    total = rx[0].astype(F32)
    for k in range(1, nr):
        total += rx[k].astype(F32)
    fr_out[...] = dot(total.astype(BF16), g[0])
    for kind in range(2):
        taken(out_sem.at[kind], sent[kind])


def store(*refs):
    held, target, store_sem = refs[:4], refs[4:8], refs[8]
    stores = [pltpu.make_async_copy(held[n], target[n], store_sem.at[n]) for n in range(4)]
    for save in stores:
        save.start()
    for save in stores:
        save.wait()


def solution(mesh):
    nr, nl = mesh.shape["region"], mesh.shape["leaf"]
    Z, Y = split_leaf(nl)

    def on_device(whiten, leaf_root, leaf_region, root_factor, root_adjoint, region_factor, region_adjoint):
        obs, K = leaf_root.shape[1], leaf_root.shape[2]
        rows = K // nl
        dma = lambda n: pltpu.SemaphoreType.DMA((max(n, 1),))
        flag = lambda n: pltpu.SemaphoreType.REGULAR((max(n, 1),))
        args = [pltpu.with_memory_space_constraint(x, pltpu.HBM) for x in (
            whiten, leaf_root, leaf_region, root_factor, root_adjoint, region_factor, region_adjoint)]
        held = pl.pallas_call(
            functools.partial(kernel, nr, nl),
            out_shape=(
                jax.ShapeDtypeStruct(leaf_root.shape, BF16),
                jax.ShapeDtypeStruct(leaf_region.shape, BF16),
                jax.ShapeDtypeStruct((rows, K), F32),
                jax.ShapeDtypeStruct((1, rows, K), F32),
            ),
            in_specs=[pl.BlockSpec(memory_space=pltpu.HBM)] * 7,
            out_specs=(pl.BlockSpec(memory_space=pltpu.VMEM),) * 4,
            scratch_shapes=[
                pltpu.VMEM((obs, obs), BF16),
                pltpu.VMEM((2, obs, K), BF16),
                pltpu.VMEM((2, obs, K), BF16),
                pltpu.VMEM((2, obs, K), BF16),
                pltpu.VMEM((2, K, K), BF16),
                pltpu.VMEM((2, K, K), BF16),
                pltpu.VMEM((2, K, K), BF16),
                pltpu.VMEM((2, Z, Y, 2, rows, K), BF16),
                pltpu.VMEM((2, Z, Y, rows, K), BF16),
                pltpu.VMEM((2, max(Y - 1, 1), Z, rows, K), BF16),
                pltpu.VMEM((2, max(Y - 1, 1), Z, rows, K), BF16),
                pltpu.VMEM((2, max(Z - 1, 1), rows, K), BF16),
                pltpu.VMEM((2, max(Z - 1, 1), rows, K), BF16),
                pltpu.VMEM((nr, rows, K), BF16),
                dma(3), dma(obs // min(256, K)), dma(2),
                dma(Z - 1), pltpu.SemaphoreType.DMA((max(Y - 1, 1), max(Z - 1, 1))), dma((Y - 1) * Z), dma(1), dma(nr - 1), dma(1), dma(2), dma(2 * Z), dma(2), dma(1),
                flag(Z - 1), flag(Y - 1), flag(1), flag(nr - 1),
            ],
            compiler_params=pltpu.CompilerParams(
                collective_id=0, has_side_effects=True, vmem_limit_bytes=40 << 20
            ),
            name="likelihood_backward",
        )(*args)
        return pl.pallas_call(
            store,
            out_shape=tuple(jax.ShapeDtypeStruct(x.shape, x.dtype) for x in held),
            in_specs=[pl.BlockSpec(memory_space=pltpu.VMEM)] * 4,
            out_specs=(pl.BlockSpec(memory_space=pltpu.HBM),) * 4,
            scratch_shapes=[dma(4)],
            compiler_params=pltpu.CompilerParams(vmem_limit_bytes=1 << 20),
            name="store_outputs",
        )(*held)

    return jax.shard_map(
        on_device,
        mesh=mesh,
        in_specs=(
            P(("region", "leaf"), None, None),
            P(("region", "leaf"), None, None),
            P(("region", "leaf"), None, None),
            P("region", None),
            P("region", None),
            P("region", "leaf", None),
            P("region", "leaf", None),
        ),
        out_specs=(
            P(("region", "leaf"), None, None),
            P(("region", "leaf"), None, None),
            P("leaf", None),
            P("region", "leaf", None),
        ),
        check_vma=False,
    )
```
